32 devices in a mesh: gx: 4 (over z), gy: 4 (over y, core), gz: 2 (over x).
Axes of the slice: x: 2, y: 2, z: 4, core: 2. Of those that a mesh axis runs over, the one named last changes fastest.
Arguments:
- coarse_source: float32 [64, 128, 256], P('gx', 'gy', 'gz'), may hold values from -6 to 6
- coarse_shift: float32 [64, 128, 256], P('gx', 'gy', 'gz'), may hold values from 0.1 to 4
- coarse_start: float32 [64, 128, 256], P('gx', 'gy', 'gz'), may hold values from -3 to 3
- fine_source: float32 [128, 32768], P(('gx', 'gy', 'gz')), may hold values from -6 to 6
- fine_shift: float32 [128, 32768], P(('gx', 'gy', 'gz')), may hold values from 0.1 to 4
- fine_start: float32 [128, 32768], P(('gx', 'gy', 'gz')), may hold values from -3 to 3
- box_corner: int32 [32, 4, 3], P(('gx', 'gy', 'gz')), may hold values from 0 to 480, as said below
- box_owner: int32 [32, 4], P(('gx', 'gy', 'gz')), may hold values from 0 to 8, as said below
Outputs:
- potential: float32 [64, 128, 256], P('gx', 'gy', 'gz')
- fine_solution: float32 [128, 32768], P(('gx', 'gy', 'gz'))
- residual_norms: float32 [2], replicated
The draws below stay inside these ranges and needn't reach their ends.
Inputs may be any that keep to these rules, and one draw needn't show every extreme that they name: `box_owner`: each device has at least one live slot; in every group of 8 devices that share a gx index some device has 4 live slots; the live owners of one device are distinct; no device is the owner of more than 4 live boxes, and in every group some device is the owner of exactly 4 live boxes. `box_corner`: each corner is a multiple of 32 and its footprint lies in the coarse block of the device that lists it; the 4 footprints of one device are distinct.
All inputs are finite; a program needn't handle non-finite values.
Results may differ from the reference program's by a relative error of at most 0.0001.
Values sent between devices are 32-bit elements; how exact they have to be, the bound alone decides.
No kernel may reach another device: no remote copies, remote signals or barrier semaphores. Data moves between devices by JAX's collectives and lax.ppermute only.
A program may use at most 128 MiB of HBM per device.

```python
import math
import jax
import jax.numpy as jnp
from jax import lax

CX = 16
CY = 32
CZ = 128
FOOT = 16
SLOTS = 4
CYCLES = 2
CSWEEPS = 4
FSWEEPS = 3
FINE = 32768
BOXES = 128
NX = 64
NY = 128
NZ = 256
N_GY = 4
N_GZ = 2
DEVICES = 32


def draw_box_owner(key, part):
    group = N_GY * N_GZ
    keys = jax.random.split(jax.random.fold_in(key, 41), DEVICES // group)

    def choose(single):
        return jax.random.permutation(single, group)[:SLOTS].astype(jnp.int32)
    offsets = jnp.repeat(jax.vmap(choose)(keys), group, axis=0)
    heavy = jnp.repeat(jax.random.randint(jax.random.fold_in(key, 42), (DEVICES // group,), 0, group).astype(jnp.int32), group)
    counts = jax.random.randint(jax.random.fold_in(key, 11), (DEVICES,), 1, SLOTS + 1).astype(jnp.int32)
    rank = jnp.arange(DEVICES, dtype=jnp.int32) % group
    senders = (heavy[:, None] - offsets) % group
    full = jnp.any(senders == rank[:, None], axis=1)
    counts = jnp.where(full, SLOTS, counts).astype(jnp.int32)
    owners = ((rank[:, None] + offsets) % group).astype(jnp.int32)
    slot = jnp.arange(SLOTS, dtype=jnp.int32)[None, :]
    return jnp.where(slot < counts[:, None], owners, group).astype(jnp.int32)


def draw_box_corner(key, part):
    group = N_GY * N_GZ
    along_x = CX // FOOT
    along_y = CY // FOOT
    along_z = CZ // FOOT
    places = along_x * along_y * along_z
    keys = jax.random.split(jax.random.fold_in(key, 31), DEVICES)

    def choose(single):
        return jax.random.permutation(single, places)[:SLOTS].astype(jnp.int32)
    picked = jax.vmap(choose)(keys)
    device = jnp.arange(DEVICES, dtype=jnp.int32)[:, None]
    device_x = device // group
    device_y = device // N_GZ % N_GY
    device_z = device % N_GZ
    block_x = picked // (along_y * along_z)
    block_y = picked // along_z % along_y
    block_z = picked % along_z
    fine_x = 2 * (device_x * CX + block_x * FOOT)
    fine_y = 2 * (device_y * CY + block_y * FOOT)
    fine_z = 2 * (device_z * CZ + block_z * FOOT)
    return jnp.stack([fine_x, fine_y, fine_z], axis=-1).astype(jnp.int32)


def block_levels(stream_key, dims, shards, low, largest):
    loudness = 1.0
    for axis_at, blocks in shards:
        steps = jax.random.uniform(jax.random.fold_in(jax.random.fold_in(stream_key, 6), axis_at), (blocks,), jnp.float32, low / len(shards), largest / len(shards))
        loudness = loudness * jnp.repeat(jnp.exp(steps), dims[axis_at] // blocks).reshape((-1,) + (1,) * (len(dims) - 1 - axis_at))
    return loudness


def noise(rng, dims, deviation, limit, cuts=(), kind=jnp.bfloat16):
    result = jax.random.normal(rng, dims, jnp.float32) * deviation
    if len(cuts) > 0:
        result = block_levels(rng, dims, cuts, -0.22, 0.18) * result
    return jnp.clip(result, min=-limit, max=limit).astype(kind)


def setup_inputs(seed: int = 0) -> dict:
    seeds = jax.random.split(jax.random.key(seed), 9)
    coarse_source = noise(seeds[0], (NX, NY, NZ), 1.0, 6.0, ((0, 4), (1, 4), (2, 2)), jnp.float32)
    coarse_shift = jnp.clip(jnp.exp(math.log(4.0) - 3.6888794 * jax.random.uniform(seeds[1], (NX, NY, NZ), jnp.float32) ** block_levels(seeds[1], (NX, NY, NZ), ((0, 4), (1, 4), (2, 2)), -0.2, 0.2)), 0.1, 4.0)
    coarse_start = noise(seeds[2], (NX, NY, NZ), 0.5, 3.0, ((0, 4), (1, 4), (2, 2)), jnp.float32)
    fine_source = noise(seeds[3], (BOXES, FINE), 1.0, 6.0, ((0, 32),), jnp.float32)
    fine_shift = jnp.clip(jnp.exp(math.log(4.0) - 3.6888794 * jax.random.uniform(seeds[4], (BOXES, FINE), jnp.float32) ** block_levels(seeds[4], (BOXES, FINE), ((0, 32),), -0.2, 0.2)), 0.1, 4.0)
    fine_start = noise(seeds[5], (BOXES, FINE), 0.5, 3.0, ((0, 32),), jnp.float32)
    box_corner = draw_box_corner(jax.random.fold_in(seeds[8], 71), 0)
    box_owner = draw_box_owner(jax.random.fold_in(seeds[8], 71), 0)
    return {"coarse_source": coarse_source, "coarse_shift": coarse_shift, "coarse_start": coarse_start, "fine_source": fine_source, "fine_shift": fine_shift, "fine_start": fine_start, "box_corner": box_corner, "box_owner": box_owner}


OMEGA = 0.8

def to_blocks(field):
    extent = field.shape
    shaped = field.reshape(extent[0] // FOOT, FOOT, extent[1] // FOOT, FOOT, extent[2] // FOOT, FOOT)
    return shaped.transpose(0, 2, 4, 1, 3, 5).reshape(-1, FOOT * FOOT * FOOT)

def from_blocks(blocks, extent):
    shaped = blocks.reshape(extent[0] // FOOT, extent[1] // FOOT, extent[2] // FOOT, FOOT, FOOT, FOOT)
    return shaped.transpose(0, 3, 1, 4, 2, 5).reshape(extent)

def inject(parents):
    number = parents.shape[0]
    shaped = parents.reshape(number, FOOT, 1, FOOT, 1, FOOT, 1)
    spread = jnp.broadcast_to(shaped, (number, FOOT, 2, FOOT, 2, FOOT, 2))
    return spread.reshape(number, 8 * FOOT * FOOT * FOOT)

def restrict(values):
    number = values.shape[0]
    return values.reshape(number, FOOT, 2, FOOT, 2, FOOT, 2).mean(axis=(2, 4, 6)).reshape(number, FOOT * FOOT * FOOT)

def fine_residual(values, parents, source, shift):
    ghost = inject(parents)
    side = 2 * FOOT
    position = jnp.arange(side * side * side, dtype=jnp.int32)[None, :]
    summed = jnp.zeros_like(values)
    for stride in (1, side, side * side):
        coordinate = position // stride % side
        upper = jnp.roll(values, -stride, axis=1)
        lower = jnp.roll(values, stride, axis=1)
        summed = summed + jnp.where(coordinate < side - 1, upper, ghost) + jnp.where(coordinate > 0, lower, ghost)
    return source - (6.0 + shift) * values + summed

def beside_sum(padded):
    summed = padded[2:, 1:-1, 1:-1] + padded[:-2, 1:-1, 1:-1]
    summed = summed + padded[1:-1, 2:, 1:-1] + padded[1:-1, :-2, 1:-1]
    return summed + padded[1:-1, 1:-1, 2:] + padded[1:-1, 1:-1, :-2]

def reference(coarse_source, coarse_shift, coarse_start, fine_source, fine_shift, fine_start, box_corner, box_owner):
    group = N_GY * N_GZ
    device_ids = jnp.arange(DEVICES, dtype=jnp.int32)
    live = box_owner < group
    owner_safe = jnp.minimum(box_owner, group - 1).astype(jnp.int32)
    hit = ((box_owner[:, :, None] == jnp.arange(group, dtype=jnp.int32)[None, None, :]) & live[:, :, None]).astype(jnp.int32)
    incoming = lax.optimization_barrier(jnp.sum(hit, axis=1)).astype(jnp.int32)
    grouped = incoming.reshape(DEVICES // group, group, group)
    before = (jnp.cumsum(grouped, axis=1).astype(jnp.int32) - grouped).reshape(DEVICES, group).astype(jnp.int32)
    slot_j = jnp.take_along_axis(before, owner_safe, axis=1).astype(jnp.int32)
    owner_global = ((device_ids // group)[:, None] * group + owner_safe).astype(jnp.int32)
    rows = (owner_global * SLOTS + slot_j).astype(jnp.int32)
    targets = jnp.where(live, rows, BOXES).reshape(-1).astype(jnp.int32)
    block = (box_corner // 2 // FOOT).reshape(-1, 3)
    block_index = ((block[:, 0] * (NY // FOOT) + block[:, 1]) * (NZ // FOOT) + block[:, 2]).astype(jnp.int32)
    home_of_row = jnp.zeros((BOXES,), jnp.int32).at[targets].set(jnp.arange(DEVICES * SLOTS, dtype=jnp.int32), mode='drop')
    occupied = jnp.zeros((BOXES,), jnp.float32).at[targets].set(1.0, mode='drop')[:, None]
    row_block = block_index[home_of_row].astype(jnp.int32)
    source = fine_source
    shift = fine_shift
    values = fine_start
    fine_diagonal = 6.0 + shift
    diagonal = 6.0 + coarse_shift
    potential = coarse_start
    earlier = None
    norms = []
    for cycle in range(CYCLES):
        parents = to_blocks(potential)[row_block]
        if cycle > 0:
            values = values + inject(parents - earlier)
        for sweep in range(FSWEEPS):
            values = values + OMEGA * fine_residual(values, parents, source, shift) / fine_diagonal
        remainder = fine_residual(values, parents, source, shift)
        restricted = restrict(remainder) * occupied
        placed = jnp.zeros((NX // FOOT * (NY // FOOT) * (NZ // FOOT), FOOT * FOOT * FOOT), jnp.float32)
        placed = placed.at[row_block].add(restricted)
        composite = coarse_source + from_blocks(placed, coarse_source.shape)
        for sweep in range(CSWEEPS):
            residual = composite - diagonal * potential + beside_sum(jnp.pad(potential, 1))
            potential = potential + OMEGA * residual / diagonal
        squares = jnp.sum(residual * residual) + jnp.sum(occupied * remainder * remainder)
        norms.append(jnp.sqrt(squares / (NX * NY * NZ)))
        earlier = parents
    parents = to_blocks(potential)[row_block]
    fine_solution = (values + inject(parents - earlier)) * occupied
    return (potential, fine_solution, jnp.stack(norms))
```

```python
import jax
import jax.numpy as jnp
from jax import lax
from jax.experimental import pallas as pl
from jax.experimental.pallas import tpu as pltpu
from jax.sharding import PartitionSpec as P

FOOT = 16
CYCLES = 2
CSWEEPS = 4
FSWEEPS = 3
OMEGA = 0.8

SUB = 8
LANES = 128
SIDE = 2 * FOOT
WIDE = 4
GROUP_AXES = ("gy", "gz")

VMEM = pl.BlockSpec(memory_space=pltpu.VMEM)
SMEM = pl.BlockSpec(memory_space=pltpu.SMEM)
F32 = jnp.float32


def out(*shape, dtype=F32):
    return jax.ShapeDtypeStruct(shape, dtype)


def call(body, name, ins, outs, scratch=(), flops=0):
    return pl.pallas_call(
        body,
        name=name,
        in_specs=[spec for spec, _ in ins],
        out_specs=[spec for spec, _ in outs],
        out_shape=[shape for _, shape in outs],
        scratch_shapes=list(scratch),
        cost_estimate=pl.CostEstimate(flops=flops, transcendentals=0, bytes_accessed=0),
    )(*[value for _, value in ins])


def lane_id():
    return lax.broadcasted_iota(jnp.int32, (SUB, LANES), 1)


def sub_id():
    return lax.broadcasted_iota(jnp.int32, (SUB, LANES), 0)


def gather(values, index, axis):
    return jnp.take_along_axis(values, index, axis=axis)


def swap_pairs(count):
    first = [(i, i ^ 1) for i in range(count)]
    second = [(i, (i + 1) % count if i % 2 else (i - 1) % count) for i in range(count)]
    return first, second


def swap(axis, first, second):
    count = lax.axis_size(axis)
    pairs_a, pairs_b = swap_pairs(count)
    got_a = lax.ppermute(first, axis, pairs_a)
    got_b = lax.ppermute(second, axis, pairs_b) if count > 2 else got_a
    return got_a, got_b


def pick_low(odd, got_a, got_b):
    return jnp.where(odd, got_a, got_b)


def pick_high(odd, got_a, got_b):
    return jnp.where(odd, got_b, got_a)


def extract(field, write, block_x, block_y, block_z):
    lanes = lane_id() // FOOT
    for quad in range(FOOT // 4):
        packed = None
        for inner in range(4):
            for part in range(FOOT // SUB):
                piece = field[FOOT * block_x + 4 * quad + inner, block_y * (FOOT // SUB) + part]
                spot = 2 * inner + part
                piece = pltpu.roll(piece, (FOOT * spot + LANES - FOOT * block_z) % LANES, 1)
                packed = piece if packed is None else jnp.where(lanes == spot, piece, packed)
        write(quad, packed)


def send_start_body(dims):
    ex, nt, group, slots, nbx, nby, nbz = dims

    def body(pos, corner, owner, start, shift, source, send, side_a, side_b):
        odd = pos[0] % 2 == 1
        for index, field in enumerate((start, shift, source)):
            low = field[0:WIDE]
            high = field[ex - WIDE : ex]
            side_a[index] = jnp.where(odd, low, high)
            side_b[index] = jnp.where(odd, high, low)
        lanes = lane_id()
        note = jnp.zeros((SUB, LANES), F32)
        blocks = []
        for slot in range(slots):
            block = (
                corner[0, slot, 0] // SIDE - pos[0] * nbx,
                corner[0, slot, 1] // SIDE - pos[1] * nby,
                corner[0, slot, 2] // SIDE - pos[2] * nbz,
            )
            blocks.append(block)
            for index, value in enumerate((owner[0, slot],) + block):
                note = jnp.where(lanes == 4 * slot + index, value.astype(F32), note)
        for target in range(group):
            send[target, 0:4] = jnp.zeros((4, SUB, LANES), F32)
            send[target, 4] = note
        for slot in range(slots):
            target = owner[0, slot]

            @pl.when(target < group)
            def _():
                def write(quad, packed):
                    send[target, quad] = packed

                extract(start, write, *blocks[slot])

    return body


def x_plane(field, got_a, got_b, odd, ex, xi):
    if xi < WIDE:
        return pick_low(odd, got_a[xi], got_b[xi])
    if xi < ex + WIDE:
        return field[xi - WIDE]
    return pick_high(odd, got_a[xi - ex - WIDE], got_b[xi - ex - WIDE])


def y_send_body(count, ex, nt):
    def body(pos, *refs):
        fields, (xa, xb, ya, yb) = refs[:count], refs[count:]
        odd_x = pos[0] % 2 == 1
        odd_y = pos[1] % 2 == 1
        for index in range(count):
            for xi in range(ex + 2 * WIDE):
                plane = x_plane(fields[index], xa.at[index], xb.at[index], odd_x, ex, xi)
                low, high = plane[0], plane[nt - 1]
                ya[index, xi] = jnp.where(odd_y, low, high)
                yb[index, xi] = jnp.where(odd_y, high, low)

    return body


def seam_tile(ya, yb, odd_y, xi):
    low = pick_low(odd_y, ya[xi], yb[xi])
    high = pick_high(odd_y, ya[xi], yb[xi])
    return jnp.where(sub_id() < WIDE, high, low)


def z_send_body(count, ex, nt, both):
    def body(pos, *refs):
        fields, refs = refs[:count], refs[count:]
        xa, xb, ya, yb = refs[:4]
        outs = refs[4:]
        odd_x = pos[0] % 2 == 1
        odd_y = pos[1] % 2 == 1
        odd_z = pos[2] % 2
        lanes = lane_id() // WIDE
        per = LANES // WIDE
        for index in range(count):
            unit = 0
            packed = [None] * len(outs)
            total = (ex + 2 * WIDE) * (nt + 1)
            for xi in range(ex + 2 * WIDE):
                plane = x_plane(fields[index], xa.at[index], xb.at[index], odd_x, ex, xi)
                for tile in range(nt + 1):
                    if tile < nt:
                        value = plane[tile]
                    else:
                        value = seam_tile(ya.at[index], yb.at[index], odd_y, xi)
                    spot = unit % per
                    for which in range(len(outs)):
                        high = 1 - odd_z if which == 0 else odd_z
                        moved = pltpu.roll(value, (WIDE * spot + WIDE * high) % LANES, 1)
                        if spot == 0:
                            packed[which] = moved
                        else:
                            packed[which] = jnp.where(lanes == spot, moved, packed[which])
                        if spot == per - 1 or unit == total - 1:
                            outs[which][index, unit // per] = packed[which]
                    unit += 1

    return body


def halo_body(count, ex, nt, both, sizes, first):
    ny_rows = SUB * nt

    def inside_xy(pos, xi, tile):
        gx = pos[0] * ex + xi - WIDE
        ok = (gx >= 0) & (gx < sizes[0] * ex)
        row = sub_id()
        if tile < nt:
            return ok, None
        y = pos[1] * ny_rows + jnp.where(row < WIDE, ny_rows + row, row - SUB)
        return ok, (y >= 0) & (y < sizes[1] * ny_rows)

    def body(pos, *refs):
        fields, refs = refs[:count], refs[count:]
        xa, xb, ya, yb = refs[:4]
        zs = refs[4 : 6 if both else 5]
        outs = refs[6 if both else 5 :]
        odd_x = pos[0] % 2 == 1
        odd_y = pos[1] % 2 == 1
        odd_z = pos[2] % 2
        lanes = lane_id()
        per = LANES // WIDE
        has_high = pos[2] < sizes[2] - 1
        has_low = pos[2] > 0
        z_mask = ((lanes < WIDE) & has_high) | ((lanes >= LANES - WIDE) & has_low)
        unit = 0
        for xi in range(ex + 2 * WIDE):
            planes = [
                x_plane(fields[index], xa.at[index], xb.at[index], odd_x, ex, xi)
                for index in range(count)
            ]
            for tile in range(nt + 1):
                ok, rows = inside_xy(pos, xi, tile)
                if rows is None:
                    good = jnp.broadcast_to(ok, (SUB, LANES))
                else:
                    good = rows & ok
                spot = unit % per
                for index in range(count):
                    if tile < nt:
                        main = planes[index][tile]
                    else:
                        main = seam_tile(ya.at[index], yb.at[index], odd_y, xi)
                    parts = []
                    for which in range(len(zs)):
                        high = 1 - odd_z if which == 0 else odd_z
                        shift = (LANES - WIDE * spot + LANES - WIDE * (1 - high)) % LANES
                        parts.append(pltpu.roll(zs[which][index, unit // per], shift, 1))
                    if len(parts) == 1:
                        halo = parts[0]
                    else:
                        halo = jnp.where(
                            lanes < LANES // 2,
                            jnp.where(odd_z == 1, parts[1], parts[0]),
                            jnp.where(odd_z == 1, parts[0], parts[1]),
                        )
                    where_main = (xi, 0, slice(SUB * tile, SUB * tile + SUB))
                    where_halo = (xi, 1, slice(SUB * tile, SUB * tile + SUB))
                    if index == 0:
                        outs[0][where_main] = jnp.where(good, main, 0.0)
                        outs[0][where_halo] = jnp.where(good & z_mask, halo, 0.0)
                    elif index == 1:
                        diag = 6.0 + main
                        outs[1][where_main] = diag
                        outs[2][where_main] = jnp.where(good, OMEGA / diag, 0.0)
                        diag = 6.0 + jnp.where(z_mask, halo, 0.0)
                        outs[1][where_halo] = diag
                        outs[2][where_halo] = jnp.where(good & z_mask, OMEGA / diag, 0.0)
                    else:
                        outs[3][where_main] = main
                        outs[3][where_halo] = jnp.where(z_mask, halo, 0.0)
                unit += 1

    return body


def around(value, ghost, masks):
    below, above, low_lanes, high_lanes, first, last = masks
    total = jnp.where(below, ghost, pltpu.roll(value, 1, 1))
    total = total + jnp.where(above, ghost, pltpu.roll(value, LANES - 1, 1))
    moved = pltpu.roll(value, SIDE, 1)
    moved = jnp.where(low_lanes, pltpu.roll(moved, 1, 0), moved)
    total = total + jnp.where(first, ghost, moved)
    moved = pltpu.roll(value, LANES - SIDE, 1)
    moved = jnp.where(high_lanes, pltpu.roll(moved, SUB - 1, 0), moved)
    return total + jnp.where(last, ghost, moved)


def fine_masks():
    lanes, rows = lane_id(), sub_id()
    low_lanes = lanes < SIDE
    high_lanes = lanes >= LANES - SIDE
    return (
        lanes % SIDE == 0,
        lanes % SIDE == SIDE - 1,
        low_lanes,
        high_lanes,
        low_lanes & (rows == 0),
        high_lanes & (rows == SUB - 1),
    )


def assign(rank, table, group, slots, found):
    count = jnp.int32(0)
    for home in range(group):
        for slot in range(slots):
            hit = table[home, 4 * slot] == rank

            @pl.when(hit)
            def _():
                found(count, home, slot)

            count = count + hit.astype(jnp.int32)
    return count


def unpack(packed, ghosts, slots):
    lanes, rows = lane_id(), sub_id()
    column = (lanes % SIDE) // 2
    row = (2 * rows + lanes // (LANES // 2)) % SUB
    upper = rows >= SUB // 2

    def box(index, carry):
        for quad in range(FOOT // 4):
            value = packed[index, quad]
            for inner in range(4):
                low = gather(value, 32 * inner + column, 1)
                high = gather(value, 32 * inner + FOOT + column, 1)
                plane = jnp.where(upper, gather(high, row, 0), gather(low, row, 0))
                ghosts[index, 4 * quad + inner] = plane
        return carry

    lax.fori_loop(0, slots, box, 0)


def fine_body(dims, first):
    group, slots, nby, nbz, size_z = dims

    def body(pos, *refs):
        if first:
            got, source, shift, start = refs[:4]
            ret, state, ghosts, squares, table = refs[4:9]
            (packed, other, diag, rate, kept, homes, copied, sems) = refs[9:]
        else:
            table, got, source, shift, old_state, old_ghosts = refs[:6]
            ret, state, ghosts, squares = refs[6:10]
            (packed, other, diag, rate, kept, homes) = refs[10:]
        rank = pos[1] * size_z + pos[2]
        if first:
            for home in range(group):
                pltpu.make_async_copy(got.at[home, 4, 0], copied.at[home], sems.at[home]).start()
        packed[...] = jnp.zeros(packed.shape, F32)

        def load(index, carry):
            for x in range(SIDE):
                at = pl.ds(SIDE * x + index, SUB, stride=slots)
                six = 6.0 + shift[at, :]
                diag[index, x] = six
                rate[index, x] = OMEGA / six
                kept[index, x] = source[at, :]
                if first:
                    other[index, 1 + x] = start[at, :]
            return carry

        lax.fori_loop(0, slots, load, 0)
        if first:
            for home in range(group):
                pltpu.make_async_copy(got.at[home, 4, 0], copied.at[home], sems.at[home]).wait()
            for home in range(group):
                for index in range(4 * slots):
                    table[home, index] = copied[home, index].astype(jnp.int32)

        def found(count, home, slot):
            packed[count] = got[home, 0:4]
            homes[count, 0] = jnp.int32(home)
            homes[count, 1] = table[home, 4 * slot + 2]
            homes[count, 2] = table[home, 4 * slot + 3]

        for slot in range(slots):
            homes[slot, 0] = jnp.int32(0)
            homes[slot, 1] = jnp.int32(0)
            homes[slot, 2] = jnp.int32(0)
        live = assign(rank, table, group, slots, found)
        unpack(packed, ghosts, slots)
        masks = fine_masks()
        lanes, rows = lane_id(), sub_id()

        def begin(index, carry):
            if not first:
                for x in range(SIDE):
                    change = ghosts[index, x // 2] - old_ghosts[index, x // 2]
                    other[index, 1 + x] = old_state[index, 1 + x] + change
            for buffer in (other, state):
                buffer[index, 0] = ghosts[index, 0]
                buffer[index, SIDE + 1] = ghosts[index, FOOT - 1]
            return carry

        lax.fori_loop(0, slots, begin, 0)

        def residual(buffer, index, x):
            value = buffer[index, 1 + x]
            near = around(value, ghosts[index, x // 2], masks)
            near = near + buffer[index, x] + buffer[index, 2 + x]
            return value, kept[index, x] - diag[index, x] * value + near

        buffers = [other, state]
        for sweep in range(FSWEEPS):
            here, there = buffers[sweep % 2], buffers[1 - sweep % 2]

            def step(index, carry):
                for x in range(SIDE):
                    value, rest = residual(here, index, x)
                    there[index, 1 + x] = value + rate[index, x] * rest
                return carry

            lax.fori_loop(0, slots, step, 0)
        final = buffers[FSWEEPS % 2]
        assert final is state

        ret_rows = [[None] * slots for _ in range(group)]

        def finish(index, total):
            zone_y = jnp.where(homes[index, 1] == 0, 0, SUB - 2)
            zone_z = jnp.where(homes[index, 2] == 0, 0, FOOT - WIDE)
            column = (rows % 2) * (LANES // 2)
            take_all = column + 2 * (lanes % FOOT)
            take_z = column + 2 * (zone_z + lanes % WIDE)
            row_y = zone_y + (rows % 4) // 2
            row_low = rows // 2
            row_high = SUB // 2 + rows // 2
            mine = jnp.zeros((SUB, LANES), F32)
            y_slab = jnp.zeros((SUB, LANES), F32)
            z_slab = jnp.zeros((SUB, LANES), F32)
            whole = None
            for xp in range(FOOT):
                value, left = residual(final, index, 2 * xp)
                mine = mine + left * left
                value, right = residual(final, index, 2 * xp + 1)
                mine = mine + right * right
                both = left + right
                both = both + pltpu.roll(both, LANES - 1, 1)
                both = 0.125 * (both + pltpu.roll(both, LANES - SIDE, 1))
                piece = gather(gather(both, row_y, 0), take_all, 1)
                y_slab = jnp.where((lanes // FOOT == xp // 2) & (rows // 4 == xp % 2), piece, y_slab)
                for part in range(2):
                    picked = gather(both, row_high if part else row_low, 0)
                    piece = gather(picked, take_all, 1)
                    spot = 2 * (xp % 4) + part
                    whole = piece if spot == 0 else jnp.where(lanes // FOOT == spot, piece, whole)
                    piece = gather(picked, take_z, 1)
                    z_slab = jnp.where(lanes // WIDE == 2 * xp + part, piece, z_slab)
                if xp % 4 == 3:
                    packed[index, xp // 4] = whole
            home_z = homes[index, 0] % size_z
            for target in range(group):
                ret[target, 4 + index] = jnp.where(home_z == target % size_z, y_slab, z_slab)
            return total + jnp.where(index < live, mine, 0.0)

        squares[...] = lax.fori_loop(0, slots, finish, jnp.zeros((SUB, LANES), F32))
        for target in range(group):
            ret[target, 0:4] = jnp.zeros((4, SUB, LANES), F32)
        for index in range(slots):

            @pl.when(index < live)
            def _():
                ret[homes[index, 0], 0:4] = packed[index]

    return body


def last_body(dims):
    group, slots, size_z = dims

    def body(pos, table, got, state, ghosts, result, packed, fresh):
        rank = pos[1] * size_z + pos[2]
        packed[...] = jnp.zeros(packed.shape, F32)

        def found(count, home, slot):
            packed[count] = got[home, 0:4]

        live = assign(rank, table, group, slots, found)
        unpack(packed, fresh, slots)

        def box(index, carry):
            for x in range(SIDE):
                value = state[index, 1 + x] + (fresh[index, x // 2] - ghosts[index, x // 2])
                value = jnp.where(index < live, value, 0.0)
                result[pl.ds(SIDE * x + index, SUB, stride=slots), :] = value
            return carry

        lax.fori_loop(0, slots, box, 0)

    return body


def place_body(dims):
    ex, nt, group, slots, size_y, size_z, nby, nbz = dims
    tiles = FOOT // SUB

    def body(pos, table, got, added, side_a, side_b):
        odd = pos[0] % 2 == 1
        rank = pos[1] * size_z + pos[2]
        lanes, rows = lane_id(), sub_id()
        added[...] = jnp.zeros(added.shape, F32)

        def slot_of(home, slot):
            owner = table[home, 4 * slot]
            count = jnp.int32(0)
            for lower in range(group):
                for index in range(slots):
                    hit = (table[lower, 4 * index] == owner) & (lower < home)
                    count = count + hit.astype(jnp.int32)
            return count

        def own(slot, carry):
            owner = table[rank, 4 * slot]

            @pl.when(owner < group)
            def _():
                base_x = FOOT * table[rank, 4 * slot + 1]
                base_y = tiles * table[rank, 4 * slot + 2]
                base_z = FOOT * table[rank, 4 * slot + 3]
                keep = (lanes >= base_z) & (lanes < base_z + FOOT)
                for quad in range(4):
                    value = got[owner, quad]
                    for inner in range(4):
                        for part in range(tiles):
                            spot = 2 * inner + part
                            moved = pltpu.roll(value, (base_z + LANES - FOOT * spot) % LANES, 1)
                            at = (base_x + 4 * quad + inner, 0, base_y + part)
                            added[at] = added[at] + jnp.where(keep, moved, 0.0)

            return carry

        lax.fori_loop(0, slots, own, 0)

        for dy in (-1, 0, 1):
            for dz in (-1, 0, 1):
                if dy == 0 and dz == 0:
                    continue
                home_y = pos[1] + dy
                home_z = pos[2] + dz
                exists = (home_y >= 0) & (home_y < size_y) & (home_z >= 0) & (home_z < size_z)
                home = jnp.where(exists, home_y * size_z + home_z, 0)

                def near(slot, carry):
                    owner = table[home, 4 * slot]
                    block_y = table[home, 4 * slot + 2]
                    block_z = table[home, 4 * slot + 3]
                    wanted = exists & (owner < group)
                    if dy != 0:
                        wanted = wanted & (block_y == (nby - 1 if dy < 0 else 0))
                    if dz != 0:
                        wanted = wanted & (block_z == (nbz - 1 if dz < 0 else 0))

                    @pl.when(wanted)
                    def _():
                        value = got[owner, 4 + slot_of(home, slot)]
                        base_x = FOOT * table[home, 4 * slot + 1]
                        goal = 0 if dy > 0 else 1
                        if dz == 0:
                            base_z = FOOT * block_z
                            keep = (lanes >= base_z) & (lanes < base_z + FOOT)
                            keep = keep & (rows // 4 == goal)
                            turned = pltpu.roll(value, 4, 0)
                            for x in range(FOOT):
                                use = value if x % 2 == goal else turned
                                shift = (base_z + LANES - FOOT * (x // 2)) % LANES
                                moved = pltpu.roll(use, shift, 1)
                                at = (base_x + x, 0, nt)
                                added[at] = added[at] + jnp.where(keep, moved, 0.0)
                        else:
                            where_z = 0 if dz > 0 else LANES - WIDE
                            keep = (lanes >= where_z) & (lanes < where_z + WIDE)
                            for x in range(FOOT):
                                for part in range(tiles):
                                    shift = (where_z + LANES - WIDE * (2 * x + part)) % LANES
                                    if dy == 0:
                                        moved = pltpu.roll(value, shift, 1)
                                        at = (base_x + x, 1, tiles * block_y + part)
                                        added[at] = added[at] + jnp.where(keep, moved, 0.0)
                                    elif part == (0 if dy > 0 else tiles - 1):
                                        moved = pltpu.roll(value, shift, 1)
                                        both = keep & (rows // 4 == goal)
                                        at = (base_x + x, 1, nt)
                                        added[at] = added[at] + jnp.where(both, moved, 0.0)

                    return carry

                lax.fori_loop(0, slots, near, 0)

        for low_side in (True, False):
            packed = None
            for index in range(WIDE - 1):
                plane = index if low_side else ex - (WIDE - 1) + index
                for tile in range(nt + 1):
                    spot = index * (nt + 1) + tile
                    moved = pltpu.roll(added[plane, 1, tile], WIDE + 2 * WIDE * spot, 1)
                    if spot == 0:
                        packed = moved
                    else:
                        packed = jnp.where(lanes // (2 * WIDE) == spot, moved, packed)
            units = (WIDE - 1) * (nt + 1)
            if low_side:
                low_packed = packed
            else:
                high_packed = packed
        for index in range(WIDE - 1):
            for tile in range(nt + 1):
                low = added[index, 0, tile]
                high = added[ex - (WIDE - 1) + index, 0, tile]
                spot = index * (nt + 1) + tile
                side_a[spot] = jnp.where(odd, low, high)
                side_b[spot] = jnp.where(odd, high, low)
        side_a[units] = jnp.where(odd, low_packed, high_packed)
        side_b[units] = jnp.where(odd, high_packed, low_packed)

    return body


def coarse_body(dims, more):
    ex, nt, group, slots, size_z = dims
    span = ex + 2 * WIDE
    rows_all = SUB * (nt + 1)

    def body(pos, table, wide, diag, rate, source, added, xa, xb, fine_sq, *refs):
        if more:
            potential, send, side_a, side_b = refs[:4]
        else:
            potential, send = refs[:2]
        comp, one, two = refs[-3:]
        odd = pos[0] % 2 == 1
        rank = pos[1] * size_z + pos[2]
        lanes = lane_id()
        halo_lanes = (lanes < WIDE) | (lanes >= LANES - WIDE)
        units = (WIDE - 1) * (nt + 1)

        def fill(x, carry):
            for zone in range(2):
                for tile in range(nt + 1):
                    at = (WIDE + x, zone, pl.ds(SUB * tile, SUB))
                    comp[at] = source[at] + added[x, zone, tile]
            return carry

        lax.fori_loop(0, ex, fill, 0)
        low_tail = pick_low(odd, xa[units], xb[units])
        high_tail = pick_high(odd, xa[units], xb[units])
        for index in range(WIDE - 1):
            for tile in range(nt + 1):
                spot = index * (nt + 1) + tile
                shift = (LANES - WIDE - 2 * WIDE * spot) % LANES
                rows = slice(SUB * tile, SUB * tile + SUB)
                xi = 1 + index
                comp[xi, 0, rows] = source[xi, 0, rows] + pick_low(odd, xa[spot], xb[spot])
                tail = jnp.where(halo_lanes, pltpu.roll(low_tail, shift, 1), 0.0)
                comp[xi, 1, rows] = source[xi, 1, rows] + tail
                xi = WIDE + ex + index
                comp[xi, 0, rows] = source[xi, 0, rows] + pick_high(odd, xa[spot], xb[spot])
                tail = jnp.where(halo_lanes, pltpu.roll(high_tail, shift, 1), 0.0)
                comp[xi, 1, rows] = source[xi, 1, rows] + tail

        edge = lax.broadcasted_iota(jnp.int32, (rows_all, LANES), 1)

        def update(here, xi):
            main, halo = here[xi, 0], here[xi, 1]
            main_up, halo_up = pltpu.roll(main, 1, 1), pltpu.roll(halo, 1, 1)
            main_dn, halo_dn = pltpu.roll(main, LANES - 1, 1), pltpu.roll(halo, LANES - 1, 1)
            at_low, at_high = edge == 0, edge == LANES - 1
            result = []
            for zone, value in ((0, main), (1, halo)):
                if zone == 0:
                    near = jnp.where(at_low, halo_up, main_up) + jnp.where(at_high, halo_dn, main_dn)
                else:
                    near = jnp.where(at_low, main_up, halo_up) + jnp.where(at_high, main_dn, halo_dn)
                near = near + pltpu.roll(value, 1, 0) + pltpu.roll(value, rows_all - 1, 0)
                near = near + here[xi - 1, zone] + here[xi + 1, zone]
                rest = comp[xi, zone] - diag[xi, zone] * value + near
                result.append((value, rest))
            return result

        buffers = [wide, one, two, one]
        for sweep in range(CSWEEPS - 1):
            here, there = buffers[sweep], buffers[sweep + 1]

            def step(xi, carry):
                for zone, (value, rest) in enumerate(update(here, xi)):
                    there[xi, zone] = value + rate[xi, zone] * rest
                return carry

            lax.fori_loop(1 + sweep, span - 1 - sweep, step, 0)
        here = buffers[CSWEEPS - 1]

        def step(x, total):
            value, rest = update(here, WIDE + x)[0]
            value = value + rate[WIDE + x, 0] * rest
            for tile in range(nt):
                rows = slice(SUB * tile, SUB * tile + SUB)
                potential[x, tile] = value[rows]
                total = total + rest[rows] * rest[rows]
            return total

        total = lax.fori_loop(0, ex, step, fine_sq[...])
        for target in range(group):
            send[target, 0:4] = jnp.zeros((4, SUB, LANES), F32)
            send[target, 4] = total
        for slot in range(slots):
            target = table[rank, 4 * slot]

            @pl.when(target < group)
            def _():
                def write(quad, packed):
                    send[target, quad] = packed

                block = [table[rank, 4 * slot + 1 + index] for index in range(3)]
                extract(potential, write, *block)

        if more:
            low = potential[0:WIDE]
            high = potential[ex - WIDE : ex]
            side_a[0] = jnp.where(odd, low, high)
            side_b[0] = jnp.where(odd, high, low)

    return body


def local(
    coarse_source,
    coarse_shift,
    coarse_start,
    fine_source,
    fine_shift,
    fine_start,
    box_corner,
    box_owner,
):
    ex, ey, ez = coarse_source.shape
    size_x, size_y, size_z = (lax.axis_size(axis) for axis in ("gx", "gy", "gz"))
    group = size_y * size_z
    slots, fine = fine_source.shape
    nbx, nby, nbz = ex // FOOT, ey // FOOT, ez // FOOT
    nt = ey // SUB
    assert ez == LANES and nby > 1 and fine == SIDE**3
    both = size_z > 2
    span = ex + 2 * WIDE
    sizes = (size_x, size_y, size_z)
    pos = jnp.stack([lax.axis_index(axis) for axis in ("gx", "gy", "gz")]).astype(jnp.int32)

    def tiled(field):
        return field.reshape(ex, nt, SUB, LANES)

    def rows(field):
        count = fine // LANES
        return field.reshape(slots, count, LANES).transpose(1, 0, 2).reshape(count * slots, LANES)

    def exchange(value):
        return lax.all_to_all(value, GROUP_AXES, split_axis=0, concat_axis=0, tiled=True)

    start, shift, source = tiled(coarse_start), tiled(coarse_shift), tiled(coarse_source)
    f_source, f_shift, f_start = rows(fine_source), rows(fine_shift), rows(fine_start)

    def halos(fields, side_a, side_b, outs, label):
        count = len(fields)
        xa, xb = swap("gx", side_a, side_b)
        ins = [(SMEM, pos)] + [(VMEM, field) for field in fields]
        ya, yb = call(
            y_send_body(count, ex, nt),
            label + "_y",
            ins + [(VMEM, xa), (VMEM, xb)],
            [(VMEM, out(count, span, SUB, LANES))] * 2,
        )
        ya, yb = swap("gy", ya, yb)
        units = -(-span * (nt + 1) // (LANES // WIDE))
        zs = call(
            z_send_body(count, ex, nt, both),
            label + "_z",
            ins + [(VMEM, value) for value in (xa, xb, ya, yb)],
            [(VMEM, out(count, units, SUB, LANES))] * (2 if both else 1),
        )
        if both:
            zs = list(swap("gz", *zs))
        else:
            zs = [swap("gz", zs[0], zs[0])[0]]
        return call(
            halo_body(count, ex, nt, both, sizes, count > 1),
            label + "_all",
            ins + [(VMEM, value) for value in (xa, xb, ya, yb, *zs)],
            [(VMEM, out(span, 2, SUB * (nt + 1), LANES))] * outs,
        )

    chunk = out(group, 5, SUB, LANES)
    send, side_a, side_b = call(
        send_start_body((ex, nt, group, slots, nbx, nby, nbz)),
        "send_start",
        [(SMEM, pos), (SMEM, box_corner), (SMEM, box_owner)]
        + [(VMEM, value) for value in (start, shift, source)],
        [(VMEM, chunk)] + [(VMEM, out(3, WIDE, nt, SUB, LANES))] * 2,
    )
    got = exchange(send)
    wide, diag, rate, source_wide = halos([start, shift, source], side_a, side_b, 4, "fixed")

    box_shape = (slots, SIDE, SUB, LANES)
    state_shape = (slots, SIDE + 2, SUB, LANES)
    box_scratch = [
        pltpu.VMEM((slots, 4, SUB, LANES), F32),
        pltpu.VMEM(state_shape, F32),
        pltpu.VMEM(box_shape, F32),
        pltpu.VMEM(box_shape, F32),
        pltpu.VMEM(box_shape, F32),
        pltpu.SMEM((slots, 3), jnp.int32),
    ]
    box_outs = [
        (VMEM, out(group, 4 + slots, SUB, LANES)),
        (VMEM, out(*state_shape)),
        (VMEM, out(slots, FOOT, SUB, LANES)),
        (VMEM, out(SUB, LANES)),
    ]
    norms = []
    table = None
    for cycle in range(CYCLES):
        first = cycle == 0
        body = fine_body((group, slots, nby, nbz, size_z), first)
        if first:
            ret, state, ghosts, squares, table = call(
                body,
                "fine_first",
                [(SMEM, pos)] + [(VMEM, value) for value in (got, f_source, f_shift, f_start)],
                box_outs + [(SMEM, out(group, 4 * slots, dtype=jnp.int32))],
                box_scratch
                + [pltpu.SMEM((group, LANES), F32), pltpu.SemaphoreType.DMA((group,))],
            )
        else:
            norms.append(jnp.sum(got[:, 4]))
            ret, state, ghosts, squares = call(
                body,
                "fine_next",
                [(SMEM, pos), (SMEM, table)]
                + [(VMEM, value) for value in (got, f_source, f_shift, state, ghosts)],
                box_outs,
                box_scratch,
            )
        back = exchange(ret)
        units = (WIDE - 1) * (nt + 1) + 1
        added, side_a, side_b = call(
            place_body((ex, nt, group, slots, size_y, size_z, nby, nbz)),
            "place",
            [(SMEM, pos), (SMEM, table), (VMEM, back)],
            [(VMEM, out(ex, 2, nt + 1, SUB, LANES))] + [(VMEM, out(units, SUB, LANES))] * 2,
        )
        xa, xb = swap("gx", side_a, side_b)
        more = cycle < CYCLES - 1
        wide_shape = (span, 2, SUB * (nt + 1), LANES)
        result = call(
            coarse_body((ex, nt, group, slots, size_z), more),
            "coarse",
            [(SMEM, pos), (SMEM, table)]
            + [(VMEM, v) for v in (wide, diag, rate, source_wide, added, xa, xb, squares)],
            [(VMEM, out(ex, nt, SUB, LANES)), (VMEM, chunk)]
            + [(VMEM, out(1, WIDE, nt, SUB, LANES))] * (2 if more else 0),
            [pltpu.VMEM(wide_shape, F32)] * 3,
        )
        potential, send = result[:2]
        got = exchange(send)
        if more:
            (wide,) = halos([potential], result[2], result[3], 1, "next")
    (values,) = call(
        last_body((group, slots, size_z)),
        "last",
        [(SMEM, pos), (SMEM, table)] + [(VMEM, value) for value in (got, state, ghosts)],
        [(VMEM, out(slots * fine // LANES, LANES))],
        [
            pltpu.VMEM((slots, 4, SUB, LANES), F32),
            pltpu.VMEM((slots, FOOT, SUB, LANES), F32),
        ],
    )
    norms.append(jnp.sum(got[:, 4]))
    total = jnp.broadcast_to(jnp.stack(norms)[None, :], (SUB, CYCLES))
    bit = 1
    while bit < size_x:
        total = total + lax.ppermute(total, "gx", [(i, i ^ bit) for i in range(size_x)])
        bit *= 2
    cells = float(ex * ey * ez * size_x * size_y * size_z)
    values = values.reshape(fine // LANES, slots, LANES).transpose(1, 0, 2).reshape(slots, fine)
    return potential.reshape(ex, ey, ez), values, jnp.sqrt(total[0] / cells)


def solution(mesh):
    in_specs = (
        P("gx", "gy", "gz"),
        P("gx", "gy", "gz"),
        P("gx", "gy", "gz"),
        P(("gx", "gy", "gz"), None),
        P(("gx", "gy", "gz"), None),
        P(("gx", "gy", "gz"), None),
        P(("gx", "gy", "gz"), None, None),
        P(("gx", "gy", "gz"), None),
    )
    out_specs = (P("gx", "gy", "gz"), P(("gx", "gy", "gz"), None), P())
    return jax.shard_map(local, mesh=mesh, in_specs=in_specs, out_specs=out_specs, check_vma=False)
```

```python
import jax
import jax.numpy as jnp
from jax import lax
from jax.experimental import pallas as pl
from jax.experimental.pallas import tpu as pltpu
from jax.sharding import PartitionSpec as P

FOOT = 16
CYCLES = 2
CSWEEPS = 4
FSWEEPS = 3
OMEGA = 0.8

SUB = 8
LANES = 128
SIDE = 2 * FOOT
WIDE = 4
GROUP_AXES = ("gy", "gz")

VMEM = pl.BlockSpec(memory_space=pltpu.VMEM)
SMEM = pl.BlockSpec(memory_space=pltpu.SMEM)
F32 = jnp.float32


def out(*shape, dtype=F32):
    return jax.ShapeDtypeStruct(shape, dtype)


def call(body, name, ins, outs, scratch=(), flops=0):
    return pl.pallas_call(
        body,
        name=name,
        in_specs=[spec for spec, _ in ins],
        out_specs=[spec for spec, _ in outs],
        out_shape=[shape for _, shape in outs],
        scratch_shapes=list(scratch),
        cost_estimate=pl.CostEstimate(flops=flops, transcendentals=0, bytes_accessed=0),
        compiler_params=pltpu.CompilerParams(vmem_limit_bytes=16 << 20),
    )(*[value for _, value in ins])


def lane_id():
    return lax.broadcasted_iota(jnp.int32, (SUB, LANES), 1)


def sub_id():
    return lax.broadcasted_iota(jnp.int32, (SUB, LANES), 0)


def gather(values, index, axis):
    return jnp.take_along_axis(values, index, axis=axis)


def swap_pairs(count):
    first = [(i, i ^ 1) for i in range(count)]
    second = [(i, (i + 1) % count if i % 2 else (i - 1) % count) for i in range(count)]
    return first, second


def swap(axis, first, second):
    count = lax.axis_size(axis)
    pairs_a, pairs_b = swap_pairs(count)
    got_a = lax.ppermute(first, axis, pairs_a)
    got_b = lax.ppermute(second, axis, pairs_b) if count > 2 else got_a
    return got_a, got_b


def pick_low(odd, got_a, got_b):
    return jnp.where(odd, got_a, got_b)


def pick_high(odd, got_a, got_b):
    return jnp.where(odd, got_b, got_a)


def extract(field, write, block_x, block_y, block_z):
    lanes = lane_id() // FOOT
    for quad in range(FOOT // 4):
        packed = None
        for inner in range(4):
            for part in range(FOOT // SUB):
                piece = field[FOOT * block_x + 4 * quad + inner, block_y * (FOOT // SUB) + part]
                spot = 2 * inner + part
                piece = pltpu.roll(piece, (FOOT * spot + LANES - FOOT * block_z) % LANES, 1)
                packed = piece if packed is None else jnp.where(lanes == spot, piece, packed)
        write(quad, packed)


def send_start_body(dims):
    ex, nt, group, slots, nbx, nby, nbz = dims

    def body(pos, corner, owner, start, shift, source, send, side_a, side_b):
        odd = pos[0] % 2 == 1
        for index, field in enumerate((start, shift, source)):
            low = field[0:WIDE]
            high = field[ex - WIDE : ex]
            side_a[index] = jnp.where(odd, low, high)
            side_b[index] = jnp.where(odd, high, low)
        lanes = lane_id()
        note = jnp.zeros((SUB, LANES), F32)
        blocks = []
        for slot in range(slots):
            block = (
                corner[0, slot, 0] // SIDE - pos[0] * nbx,
                corner[0, slot, 1] // SIDE - pos[1] * nby,
                corner[0, slot, 2] // SIDE - pos[2] * nbz,
            )
            blocks.append(block)
            for index, value in enumerate((owner[0, slot],) + block):
                note = jnp.where(lanes == 4 * slot + index, value.astype(F32), note)
        for target in range(group):
            send[target, 0:4] = jnp.zeros((4, SUB, LANES), F32)
            send[target, 4] = note
        for slot in range(slots):
            target = owner[0, slot]

            @pl.when(target < group)
            def _():
                def write(quad, packed):
                    send[target, quad] = packed

                extract(start, write, *blocks[slot])

    return body


def x_plane(field, got_a, got_b, odd, ex, xi):
    if xi < WIDE:
        return pick_low(odd, got_a[xi], got_b[xi])
    if xi < ex + WIDE:
        return field[xi - WIDE]
    return pick_high(odd, got_a[xi - ex - WIDE], got_b[xi - ex - WIDE])


def y_send_body(count, ex, nt):
    def body(pos, *refs):
        fields, (xa, xb, ya, yb) = refs[:count], refs[count:]
        odd_x = pos[0] % 2 == 1
        odd_y = pos[1] % 2 == 1
        for index in range(count):
            for xi in range(ex + 2 * WIDE):
                plane = x_plane(fields[index], xa.at[index], xb.at[index], odd_x, ex, xi)
                low, high = plane[0], plane[nt - 1]
                ya[index, xi] = jnp.where(odd_y, low, high)
                yb[index, xi] = jnp.where(odd_y, high, low)

    return body


def seam_tile(ya, yb, odd_y, xi):
    low = pick_low(odd_y, ya[xi], yb[xi])
    high = pick_high(odd_y, ya[xi], yb[xi])
    return jnp.where(sub_id() < WIDE, high, low)


def z_send_body(count, ex, nt, both):
    def body(pos, *refs):
        fields, refs = refs[:count], refs[count:]
        xa, xb, ya, yb = refs[:4]
        outs = refs[4:]
        odd_x = pos[0] % 2 == 1
        odd_y = pos[1] % 2 == 1
        odd_z = pos[2] % 2
        lanes = lane_id() // WIDE
        per = LANES // WIDE
        for index in range(count):
            unit = 0
            packed = [None] * len(outs)
            total = (ex + 2 * WIDE) * (nt + 1)
            for xi in range(ex + 2 * WIDE):
                plane = x_plane(fields[index], xa.at[index], xb.at[index], odd_x, ex, xi)
                for tile in range(nt + 1):
                    if tile < nt:
                        value = plane[tile]
                    else:
                        value = seam_tile(ya.at[index], yb.at[index], odd_y, xi)
                    spot = unit % per
                    for which in range(len(outs)):
                        high = 1 - odd_z if which == 0 else odd_z
                        moved = pltpu.roll(value, (WIDE * spot + WIDE * high) % LANES, 1)
                        if spot == 0:
                            packed[which] = moved
                        else:
                            packed[which] = jnp.where(lanes == spot, moved, packed[which])
                        if spot == per - 1 or unit == total - 1:
                            outs[which][index, unit // per] = packed[which]
                    unit += 1

    return body


def halo_body(count, ex, nt, both, sizes, first):
    ny_rows = SUB * nt

    def inside_xy(pos, xi, tile):
        gx = pos[0] * ex + xi - WIDE
        ok = (gx >= 0) & (gx < sizes[0] * ex)
        row = sub_id()
        if tile < nt:
            return ok, None
        y = pos[1] * ny_rows + jnp.where(row < WIDE, ny_rows + row, row - SUB)
        return ok, (y >= 0) & (y < sizes[1] * ny_rows)

    def body(pos, *refs):
        fields, refs = refs[:count], refs[count:]
        xa, xb, ya, yb = refs[:4]
        zs = refs[4 : 6 if both else 5]
        outs = refs[6 if both else 5 :]
        odd_x = pos[0] % 2 == 1
        odd_y = pos[1] % 2 == 1
        odd_z = pos[2] % 2
        lanes = lane_id()
        per = LANES // WIDE
        has_high = pos[2] < sizes[2] - 1
        has_low = pos[2] > 0
        z_mask = ((lanes < WIDE) & has_high) | ((lanes >= LANES - WIDE) & has_low)
        unit = 0
        for xi in range(ex + 2 * WIDE):
            planes = [
                x_plane(fields[index], xa.at[index], xb.at[index], odd_x, ex, xi)
                for index in range(count)
            ]
            for tile in range(nt + 1):
                ok, rows = inside_xy(pos, xi, tile)
                if rows is None:
                    good = jnp.broadcast_to(ok, (SUB, LANES))
                else:
                    good = rows & ok
                spot = unit % per
                for index in range(count):
                    if tile < nt:
                        main = planes[index][tile]
                    else:
                        main = seam_tile(ya.at[index], yb.at[index], odd_y, xi)
                    parts = []
                    for which in range(len(zs)):
                        high = 1 - odd_z if which == 0 else odd_z
                        shift = (LANES - WIDE * spot + LANES - WIDE * (1 - high)) % LANES
                        parts.append(pltpu.roll(zs[which][index, unit // per], shift, 1))
                    if len(parts) == 1:
                        halo = parts[0]
                    else:
                        halo = jnp.where(
                            lanes < LANES // 2,
                            jnp.where(odd_z == 1, parts[1], parts[0]),
                            jnp.where(odd_z == 1, parts[0], parts[1]),
                        )
                    where_main = (xi, 0, slice(SUB * tile, SUB * tile + SUB))
                    where_halo = (xi, 1, slice(SUB * tile, SUB * tile + SUB))
                    if index == 0:
                        outs[0][where_main] = jnp.where(good, main, 0.0)
                        outs[0][where_halo] = jnp.where(good & z_mask, halo, 0.0)
                    elif index == 1:
                        diag = 6.0 + main
                        outs[1][where_main] = diag
                        outs[2][where_main] = jnp.where(good, OMEGA / diag, 0.0)
                        diag = 6.0 + jnp.where(z_mask, halo, 0.0)
                        outs[1][where_halo] = diag
                        outs[2][where_halo] = jnp.where(good & z_mask, OMEGA / diag, 0.0)
                    else:
                        outs[3][where_main] = main
                        outs[3][where_halo] = jnp.where(z_mask, halo, 0.0)
                unit += 1

    return body


def around(value, ghost, masks):
    below, above, low_lanes, high_lanes, first, last = masks
    total = jnp.where(below, ghost, pltpu.roll(value, 1, 1))
    total = total + jnp.where(above, ghost, pltpu.roll(value, LANES - 1, 1))
    moved = pltpu.roll(value, SIDE, 1)
    moved = jnp.where(low_lanes, pltpu.roll(moved, 1, 0), moved)
    total = total + jnp.where(first, ghost, moved)
    moved = pltpu.roll(value, LANES - SIDE, 1)
    moved = jnp.where(high_lanes, pltpu.roll(moved, SUB - 1, 0), moved)
    return total + jnp.where(last, ghost, moved)


def fine_masks():
    lanes, rows = lane_id(), sub_id()
    low_lanes = lanes < SIDE
    high_lanes = lanes >= LANES - SIDE
    return (
        lanes % SIDE == 0,
        lanes % SIDE == SIDE - 1,
        low_lanes,
        high_lanes,
        low_lanes & (rows == 0),
        high_lanes & (rows == SUB - 1),
    )


def assign(rank, table, group, slots, found):
    count = jnp.int32(0)
    for home in range(group):
        for slot in range(slots):
            hit = table[home, 4 * slot] == rank

            @pl.when(hit)
            def _():
                found(count, home, slot)

            count = count + hit.astype(jnp.int32)
    return count


def unpack(packed, ghosts, slots):
    lanes, rows = lane_id(), sub_id()
    column = (lanes % SIDE) // 2
    row = (2 * rows + lanes // (LANES // 2)) % SUB
    upper = rows >= SUB // 2

    def box(index, carry):
        for quad in range(FOOT // 4):
            value = packed[index, quad]
            for inner in range(4):
                low = gather(value, 32 * inner + column, 1)
                high = gather(value, 32 * inner + FOOT + column, 1)
                plane = jnp.where(upper, gather(high, row, 0), gather(low, row, 0))
                ghosts[index, 4 * quad + inner] = plane
        return carry

    lax.fori_loop(0, slots, box, 0)


def fine_body(dims, first):
    group, slots, nby, nbz, size_z = dims

    def body(pos, *refs):
        if first:
            got, source, shift, start = refs[:4]
            ret, state, ghosts, squares, table = refs[4:9]
            (packed, other, diag, rate, kept, homes, copied, sems) = refs[9:]
        else:
            table, got, source, shift, old_state, old_ghosts = refs[:6]
            ret, state, ghosts, squares = refs[6:10]
            (packed, other, diag, rate, kept, homes) = refs[10:]
        rank = pos[1] * size_z + pos[2]
        if first:
            for home in range(group):
                pltpu.make_async_copy(got.at[home, 4, 0], copied.at[home], sems.at[home]).start()
        packed[...] = jnp.zeros(packed.shape, F32)

        def load(index, carry):
            for x in range(SIDE):
                at = pl.ds(SIDE * x + index, SUB, stride=slots)
                six = 6.0 + shift[at, :]
                diag[index, x] = six
                rate[index, x] = OMEGA / six
                kept[index, x] = source[at, :]
                if first:
                    other[index, 1 + x] = start[at, :]
            return carry

        lax.fori_loop(0, slots, load, 0)
        if first:
            for home in range(group):
                pltpu.make_async_copy(got.at[home, 4, 0], copied.at[home], sems.at[home]).wait()
            for home in range(group):
                for index in range(4 * slots):
                    table[home, index] = copied[home, index].astype(jnp.int32)

        def found(count, home, slot):
            packed[count] = got[home, 0:4]
            homes[count, 0] = jnp.int32(home)
            homes[count, 1] = table[home, 4 * slot + 2]
            homes[count, 2] = table[home, 4 * slot + 3]

        for slot in range(slots):
            homes[slot, 0] = jnp.int32(0)
            homes[slot, 1] = jnp.int32(0)
            homes[slot, 2] = jnp.int32(0)
        live = assign(rank, table, group, slots, found)
        unpack(packed, ghosts, slots)
        masks = fine_masks()
        lanes, rows = lane_id(), sub_id()

        def begin(index, carry):
            if not first:
                for x in range(SIDE):
                    change = ghosts[index, x // 2] - old_ghosts[index, x // 2]
                    other[index, 1 + x] = old_state[index, 1 + x] + change
            for buffer in (other, state):
                buffer[index, 0] = ghosts[index, 0]
                buffer[index, SIDE + 1] = ghosts[index, FOOT - 1]
            return carry

        lax.fori_loop(0, slots, begin, 0)

        def residual(buffer, index, x):
            value = buffer[index, 1 + x]
            near = around(value, ghosts[index, x // 2], masks)
            near = near + buffer[index, x] + buffer[index, 2 + x]
            return value, kept[index, x] - diag[index, x] * value + near

        buffers = [other, state]
        for sweep in range(FSWEEPS):
            here, there = buffers[sweep % 2], buffers[1 - sweep % 2]

            def step(index, carry):
                for x in range(SIDE):
                    value, rest = residual(here, index, x)
                    there[index, 1 + x] = value + rate[index, x] * rest
                return carry

            lax.fori_loop(0, slots, step, 0)
        final = buffers[FSWEEPS % 2]
        assert final is state

        ret_rows = [[None] * slots for _ in range(group)]

        def finish(index, total):
            zone_y = jnp.where(homes[index, 1] == 0, 0, SUB - 2)
            zone_z = jnp.where(homes[index, 2] == 0, 0, FOOT - WIDE)
            column = (rows % 2) * (LANES // 2)
            take_all = column + 2 * (lanes % FOOT)
            take_z = column + 2 * (zone_z + lanes % WIDE)
            row_y = zone_y + (rows % 4) // 2
            row_low = rows // 2
            row_high = SUB // 2 + rows // 2
            mine = jnp.zeros((SUB, LANES), F32)
            y_slab = jnp.zeros((SUB, LANES), F32)
            z_slab = jnp.zeros((SUB, LANES), F32)
            whole = None
            for xp in range(FOOT):
                value, left = residual(final, index, 2 * xp)
                mine = mine + left * left
                value, right = residual(final, index, 2 * xp + 1)
                mine = mine + right * right
                both = left + right
                both = both + pltpu.roll(both, LANES - 1, 1)
                both = 0.125 * (both + pltpu.roll(both, LANES - SIDE, 1))
                piece = gather(gather(both, row_y, 0), take_all, 1)
                y_slab = jnp.where((lanes // FOOT == xp // 2) & (rows // 4 == xp % 2), piece, y_slab)
                for part in range(2):
                    picked = gather(both, row_high if part else row_low, 0)
                    piece = gather(picked, take_all, 1)
                    spot = 2 * (xp % 4) + part
                    whole = piece if spot == 0 else jnp.where(lanes // FOOT == spot, piece, whole)
                    piece = gather(picked, take_z, 1)
                    z_slab = jnp.where(lanes // WIDE == 2 * xp + part, piece, z_slab)
                if xp % 4 == 3:
                    packed[index, xp // 4] = whole
            home_z = homes[index, 0] % size_z
            for target in range(group):
                ret[target, 4 + index] = jnp.where(home_z == target % size_z, y_slab, z_slab)
            return total + jnp.where(index < live, mine, 0.0)

        squares[...] = lax.fori_loop(0, slots, finish, jnp.zeros((SUB, LANES), F32))
        for target in range(group):
            ret[target, 0:4] = jnp.zeros((4, SUB, LANES), F32)
        for index in range(slots):

            @pl.when(index < live)
            def _():
                ret[homes[index, 0], 0:4] = packed[index]

    return body


def last_body(dims):
    group, slots, size_z = dims

    def body(pos, table, got, state, ghosts, result, packed, fresh):
        rank = pos[1] * size_z + pos[2]
        packed[...] = jnp.zeros(packed.shape, F32)

        def found(count, home, slot):
            packed[count] = got[home, 0:4]

        live = assign(rank, table, group, slots, found)
        unpack(packed, fresh, slots)

        def box(index, carry):
            for x in range(SIDE):
                value = state[index, 1 + x] + (fresh[index, x // 2] - ghosts[index, x // 2])
                value = jnp.where(index < live, value, 0.0)
                result[pl.ds(SIDE * x + index, SUB, stride=slots), :] = value
            return carry

        lax.fori_loop(0, slots, box, 0)

    return body


def place_body(dims):
    ex, nt, group, slots, size_y, size_z, nby, nbz = dims
    tiles = FOOT // SUB

    def body(pos, table, got, added, side_a, side_b):
        odd = pos[0] % 2 == 1
        rank = pos[1] * size_z + pos[2]
        lanes, rows = lane_id(), sub_id()
        added[...] = jnp.zeros(added.shape, F32)

        def slot_of(home, slot):
            owner = table[home, 4 * slot]
            count = jnp.int32(0)
            for lower in range(group):
                for index in range(slots):
                    hit = (table[lower, 4 * index] == owner) & (lower < home)
                    count = count + hit.astype(jnp.int32)
            return count

        def own(slot, carry):
            owner = table[rank, 4 * slot]

            @pl.when(owner < group)
            def _():
                base_x = FOOT * table[rank, 4 * slot + 1]
                base_y = tiles * table[rank, 4 * slot + 2]
                base_z = FOOT * table[rank, 4 * slot + 3]
                keep = (lanes >= base_z) & (lanes < base_z + FOOT)
                for quad in range(4):
                    value = got[owner, quad]
                    for inner in range(4):
                        for part in range(tiles):
                            spot = 2 * inner + part
                            moved = pltpu.roll(value, (base_z + LANES - FOOT * spot) % LANES, 1)
                            at = (base_x + 4 * quad + inner, 0, base_y + part)
                            added[at] = added[at] + jnp.where(keep, moved, 0.0)

            return carry

        lax.fori_loop(0, slots, own, 0)

        for dy in (-1, 0, 1):
            for dz in (-1, 0, 1):
                if dy == 0 and dz == 0:
                    continue
                home_y = pos[1] + dy
                home_z = pos[2] + dz
                exists = (home_y >= 0) & (home_y < size_y) & (home_z >= 0) & (home_z < size_z)
                home = jnp.where(exists, home_y * size_z + home_z, 0)

                def near(slot, carry):
                    owner = table[home, 4 * slot]
                    block_y = table[home, 4 * slot + 2]
                    block_z = table[home, 4 * slot + 3]
                    wanted = exists & (owner < group)
                    if dy != 0:
                        wanted = wanted & (block_y == (nby - 1 if dy < 0 else 0))
                    if dz != 0:
                        wanted = wanted & (block_z == (nbz - 1 if dz < 0 else 0))

                    @pl.when(wanted)
                    def _():
                        value = got[owner, 4 + slot_of(home, slot)]
                        base_x = FOOT * table[home, 4 * slot + 1]
                        goal = 0 if dy > 0 else 1
                        if dz == 0:
                            base_z = FOOT * block_z
                            keep = (lanes >= base_z) & (lanes < base_z + FOOT)
                            keep = keep & (rows // 4 == goal)
                            turned = pltpu.roll(value, 4, 0)
                            for x in range(FOOT):
                                use = value if x % 2 == goal else turned
                                shift = (base_z + LANES - FOOT * (x // 2)) % LANES
                                moved = pltpu.roll(use, shift, 1)
                                at = (base_x + x, 0, nt)
                                added[at] = added[at] + jnp.where(keep, moved, 0.0)
                        else:
                            where_z = 0 if dz > 0 else LANES - WIDE
                            keep = (lanes >= where_z) & (lanes < where_z + WIDE)
                            for x in range(FOOT):
                                for part in range(tiles):
                                    shift = (where_z + LANES - WIDE * (2 * x + part)) % LANES
                                    if dy == 0:
                                        moved = pltpu.roll(value, shift, 1)
                                        at = (base_x + x, 1, tiles * block_y + part)
                                        added[at] = added[at] + jnp.where(keep, moved, 0.0)
                                    elif part == (0 if dy > 0 else tiles - 1):
                                        moved = pltpu.roll(value, shift, 1)
                                        both = keep & (rows // 4 == goal)
                                        at = (base_x + x, 1, nt)
                                        added[at] = added[at] + jnp.where(both, moved, 0.0)

                    return carry

                lax.fori_loop(0, slots, near, 0)

        for low_side in (True, False):
            packed = None
            for index in range(WIDE - 1):
                plane = index if low_side else ex - (WIDE - 1) + index
                for tile in range(nt + 1):
                    spot = index * (nt + 1) + tile
                    moved = pltpu.roll(added[plane, 1, tile], WIDE + 2 * WIDE * spot, 1)
                    if spot == 0:
                        packed = moved
                    else:
                        packed = jnp.where(lanes // (2 * WIDE) == spot, moved, packed)
            units = (WIDE - 1) * (nt + 1)
            if low_side:
                low_packed = packed
            else:
                high_packed = packed
        for index in range(WIDE - 1):
            for tile in range(nt + 1):
                low = added[index, 0, tile]
                high = added[ex - (WIDE - 1) + index, 0, tile]
                spot = index * (nt + 1) + tile
                side_a[spot] = jnp.where(odd, low, high)
                side_b[spot] = jnp.where(odd, high, low)
        side_a[units] = jnp.where(odd, low_packed, high_packed)
        side_b[units] = jnp.where(odd, high_packed, low_packed)

    return body


def coarse_body(dims, more):
    ex, nt, group, slots, size_z = dims
    span = ex + 2 * WIDE
    rows_all = SUB * (nt + 1)

    def body(pos, table, wide, diag, rate, source, added, xa, xb, fine_sq, *refs):
        if more:
            potential, send, side_a, side_b = refs[:4]
        else:
            potential, send = refs[:2]
        comp, one, two = refs[-3:]
        odd = pos[0] % 2 == 1
        rank = pos[1] * size_z + pos[2]
        lanes = lane_id()
        halo_lanes = (lanes < WIDE) | (lanes >= LANES - WIDE)
        units = (WIDE - 1) * (nt + 1)

        def fill(x, carry):
            for zone in range(2):
                for tile in range(nt + 1):
                    at = (WIDE + x, zone, pl.ds(SUB * tile, SUB))
                    comp[at] = source[at] + added[x, zone, tile]
            return carry

        lax.fori_loop(0, ex, fill, 0)
        low_tail = pick_low(odd, xa[units], xb[units])
        high_tail = pick_high(odd, xa[units], xb[units])
        for index in range(WIDE - 1):
            for tile in range(nt + 1):
                spot = index * (nt + 1) + tile
                shift = (LANES - WIDE - 2 * WIDE * spot) % LANES
                rows = slice(SUB * tile, SUB * tile + SUB)
                xi = 1 + index
                comp[xi, 0, rows] = source[xi, 0, rows] + pick_low(odd, xa[spot], xb[spot])
                tail = jnp.where(halo_lanes, pltpu.roll(low_tail, shift, 1), 0.0)
                comp[xi, 1, rows] = source[xi, 1, rows] + tail
                xi = WIDE + ex + index
                comp[xi, 0, rows] = source[xi, 0, rows] + pick_high(odd, xa[spot], xb[spot])
                tail = jnp.where(halo_lanes, pltpu.roll(high_tail, shift, 1), 0.0)
                comp[xi, 1, rows] = source[xi, 1, rows] + tail

        edge = lax.broadcasted_iota(jnp.int32, (rows_all, LANES), 1)

        def update(here, xi):
            main, halo = here[xi, 0], here[xi, 1]
            main_up, halo_up = pltpu.roll(main, 1, 1), pltpu.roll(halo, 1, 1)
            main_dn, halo_dn = pltpu.roll(main, LANES - 1, 1), pltpu.roll(halo, LANES - 1, 1)
            at_low, at_high = edge == 0, edge == LANES - 1
            result = []
            for zone, value in ((0, main), (1, halo)):
                if zone == 0:
                    near = jnp.where(at_low, halo_up, main_up) + jnp.where(at_high, halo_dn, main_dn)
                else:
                    near = jnp.where(at_low, main_up, halo_up) + jnp.where(at_high, main_dn, halo_dn)
                near = near + pltpu.roll(value, 1, 0) + pltpu.roll(value, rows_all - 1, 0)
                near = near + here[xi - 1, zone] + here[xi + 1, zone]
                rest = comp[xi, zone] - diag[xi, zone] * value + near
                result.append((value, rest))
            return result

        buffers = [wide, one, two, one]
        for sweep in range(CSWEEPS - 1):
            here, there = buffers[sweep], buffers[sweep + 1]

            def step(xi, carry):
                for zone, (value, rest) in enumerate(update(here, xi)):
                    there[xi, zone] = value + rate[xi, zone] * rest
                return carry

            lax.fori_loop(1 + sweep, span - 1 - sweep, step, 0)
        here = buffers[CSWEEPS - 1]

        def step(x, total):
            value, rest = update(here, WIDE + x)[0]
            value = value + rate[WIDE + x, 0] * rest
            for tile in range(nt):
                rows = slice(SUB * tile, SUB * tile + SUB)
                potential[x, tile] = value[rows]
                total = total + rest[rows] * rest[rows]
            return total

        total = lax.fori_loop(0, ex, step, fine_sq[...])
        for target in range(group):
            send[target, 0:4] = jnp.zeros((4, SUB, LANES), F32)
            send[target, 4] = total
        for slot in range(slots):
            target = table[rank, 4 * slot]

            @pl.when(target < group)
            def _():
                def write(quad, packed):
                    send[target, quad] = packed

                block = [table[rank, 4 * slot + 1 + index] for index in range(3)]
                extract(potential, write, *block)

        if more:
            low = potential[0:WIDE]
            high = potential[ex - WIDE : ex]
            side_a[0] = jnp.where(odd, low, high)
            side_b[0] = jnp.where(odd, high, low)

    return body


def local(
    coarse_source,
    coarse_shift,
    coarse_start,
    fine_source,
    fine_shift,
    fine_start,
    box_corner,
    box_owner,
):
    ex, ey, ez = coarse_source.shape
    size_x, size_y, size_z = (lax.axis_size(axis) for axis in ("gx", "gy", "gz"))
    group = size_y * size_z
    slots, fine = fine_source.shape
    nbx, nby, nbz = ex // FOOT, ey // FOOT, ez // FOOT
    nt = ey // SUB
    assert ez == LANES and nby > 1 and fine == SIDE**3
    both = size_z > 2
    span = ex + 2 * WIDE
    sizes = (size_x, size_y, size_z)
    pos = jnp.stack([lax.axis_index(axis) for axis in ("gx", "gy", "gz")]).astype(jnp.int32)

    def tiled(field):
        return field.reshape(ex, nt, SUB, LANES)

    def rows(field):
        count = fine // LANES
        return field.reshape(slots, count, LANES).transpose(1, 0, 2).reshape(count * slots, LANES)

    def exchange(value):
        return lax.all_to_all(value, GROUP_AXES, split_axis=0, concat_axis=0, tiled=True)

    start, shift, source = tiled(coarse_start), tiled(coarse_shift), tiled(coarse_source)
    f_source, f_shift, f_start = rows(fine_source), rows(fine_shift), rows(fine_start)

    def halos(fields, side_a, side_b, outs, label):
        count = len(fields)
        xa, xb = swap("gx", side_a, side_b)
        ins = [(SMEM, pos)] + [(VMEM, field) for field in fields]
        ya, yb = call(
            y_send_body(count, ex, nt),
            label + "_y",
            ins + [(VMEM, xa), (VMEM, xb)],
            [(VMEM, out(count, span, SUB, LANES))] * 2,
        )
        ya, yb = swap("gy", ya, yb)
        units = -(-span * (nt + 1) // (LANES // WIDE))
        zs = call(
            z_send_body(count, ex, nt, both),
            label + "_z",
            ins + [(VMEM, value) for value in (xa, xb, ya, yb)],
            [(VMEM, out(count, units, SUB, LANES))] * (2 if both else 1),
        )
        if both:
            zs = list(swap("gz", *zs))
        else:
            zs = [swap("gz", zs[0], zs[0])[0]]
        return call(
            halo_body(count, ex, nt, both, sizes, count > 1),
            label + "_all",
            ins + [(VMEM, value) for value in (xa, xb, ya, yb, *zs)],
            [(VMEM, out(span, 2, SUB * (nt + 1), LANES))] * outs,
        )

    chunk = out(group, 5, SUB, LANES)
    send, side_a, side_b = call(
        send_start_body((ex, nt, group, slots, nbx, nby, nbz)),
        "send_start",
        [(SMEM, pos), (SMEM, box_corner), (SMEM, box_owner)]
        + [(VMEM, value) for value in (start, shift, source)],
        [(VMEM, chunk)] + [(VMEM, out(3, WIDE, nt, SUB, LANES))] * 2,
    )
    got = exchange(send)
    wide, diag, rate, source_wide = halos([start, shift, source], side_a, side_b, 4, "fixed")

    box_shape = (slots, SIDE, SUB, LANES)
    state_shape = (slots, SIDE + 2, SUB, LANES)
    box_scratch = [
        pltpu.VMEM((slots, 4, SUB, LANES), F32),
        pltpu.VMEM(state_shape, F32),
        pltpu.VMEM(box_shape, F32),
        pltpu.VMEM(box_shape, F32),
        pltpu.VMEM(box_shape, F32),
        pltpu.SMEM((slots, 3), jnp.int32),
    ]
    box_outs = [
        (VMEM, out(group, 4 + slots, SUB, LANES)),
        (VMEM, out(*state_shape)),
        (VMEM, out(slots, FOOT, SUB, LANES)),
        (VMEM, out(SUB, LANES)),
    ]
    norms = []
    table = None
    for cycle in range(CYCLES):
        first = cycle == 0
        body = fine_body((group, slots, nby, nbz, size_z), first)
        if first:
            ret, state, ghosts, squares, table = call(
                body,
                "fine_first",
                [(SMEM, pos)] + [(VMEM, value) for value in (got, f_source, f_shift, f_start)],
                box_outs + [(SMEM, out(group, 4 * slots, dtype=jnp.int32))],
                box_scratch
                + [pltpu.SMEM((group, LANES), F32), pltpu.SemaphoreType.DMA((group,))],
            )
        else:
            norms.append(jnp.sum(got[:, 4]))
            ret, state, ghosts, squares = call(
                body,
                "fine_next",
                [(SMEM, pos), (SMEM, table)]
                + [(VMEM, value) for value in (got, f_source, f_shift, state, ghosts)],
                box_outs,
                box_scratch,
            )
        back = exchange(ret)
        units = (WIDE - 1) * (nt + 1) + 1
        added, side_a, side_b = call(
            place_body((ex, nt, group, slots, size_y, size_z, nby, nbz)),
            "place",
            [(SMEM, pos), (SMEM, table), (VMEM, back)],
            [(VMEM, out(ex, 2, nt + 1, SUB, LANES))] + [(VMEM, out(units, SUB, LANES))] * 2,
        )
        xa, xb = swap("gx", side_a, side_b)
        more = cycle < CYCLES - 1
        wide_shape = (span, 2, SUB * (nt + 1), LANES)
        result = call(
            coarse_body((ex, nt, group, slots, size_z), more),
            "coarse",
            [(SMEM, pos), (SMEM, table)]
            + [(VMEM, v) for v in (wide, diag, rate, source_wide, added, xa, xb, squares)],
            [(VMEM, out(ex, nt, SUB, LANES)), (VMEM, chunk)]
            + [(VMEM, out(1, WIDE, nt, SUB, LANES))] * (2 if more else 0),
            [pltpu.VMEM(wide_shape, F32)] * 3,
        )
        potential, send = result[:2]
        got = exchange(send)
        if more:
            (wide,) = halos([potential], result[2], result[3], 1, "next")
    (values,) = call(
        last_body((group, slots, size_z)),
        "last",
        [(SMEM, pos), (SMEM, table)] + [(VMEM, value) for value in (got, state, ghosts)],
        [(VMEM, out(slots * fine // LANES, LANES))],
        [
            pltpu.VMEM((slots, 4, SUB, LANES), F32),
            pltpu.VMEM((slots, FOOT, SUB, LANES), F32),
        ],
    )
    norms.append(jnp.sum(got[:, 4]))
    total = jnp.broadcast_to(jnp.stack(norms)[None, :], (SUB, CYCLES))
    bit = 1
    while bit < size_x:
        total = total + lax.ppermute(total, "gx", [(i, i ^ bit) for i in range(size_x)])
        bit *= 2
    cells = float(ex * ey * ez * size_x * size_y * size_z)
    values = values.reshape(fine // LANES, slots, LANES).transpose(1, 0, 2).reshape(slots, fine)
    return potential.reshape(ex, ey, ez), values, jnp.sqrt(total[0] / cells)


def solution(mesh):
    in_specs = (
        P("gx", "gy", "gz"),
        P("gx", "gy", "gz"),
        P("gx", "gy", "gz"),
        P(("gx", "gy", "gz"), None),
        P(("gx", "gy", "gz"), None),
        P(("gx", "gy", "gz"), None),
        P(("gx", "gy", "gz"), None, None),
        P(("gx", "gy", "gz"), None),
    )
    out_specs = (P("gx", "gy", "gz"), P(("gx", "gy", "gz"), None), P())
    return jax.shard_map(local, mesh=mesh, in_specs=in_specs, out_specs=out_specs, check_vma=False)
```

```python
import jax
import jax.numpy as jnp
from jax import lax
from jax.experimental import pallas as pl
from jax.experimental.pallas import tpu as pltpu
from jax.sharding import PartitionSpec as P


FOOT = 16
CYCLES = 2
CSWEEPS = 4
FSWEEPS = 3
OMEGA = 0.8

SUB = 8
LANES = 128
SIDE = 2 * FOOT
WIDE = 4
COLS = 8
GROUP_AXES = ("gy", "gz")

VMEM = pl.BlockSpec(memory_space=pltpu.VMEM)
SMEM = pl.BlockSpec(memory_space=pltpu.SMEM)
HBM = pl.BlockSpec(memory_space=pltpu.HBM)
F32 = jnp.float32


def out(*shape, dtype=F32):
    return jax.ShapeDtypeStruct(shape, dtype)


def call(body, ins, outs, scratch=()):
    values = [
        pltpu.with_memory_space_constraint(value, pltpu.HBM) if spec is HBM else value
        for spec, value in ins
    ]
    shapes = [pltpu.HBM(shape.shape, shape.dtype) if spec is HBM else shape for spec, shape in outs]
    return pl.pallas_call(
        body,
        in_specs=[spec for spec, _ in ins],
        out_specs=[spec for spec, _ in outs],
        out_shape=shapes,
        scratch_shapes=list(scratch),
        compiler_params=pltpu.CompilerParams(vmem_limit_bytes=16 << 20),
    )(*values)


def place_of():
    return [lax.axis_index(axis) for axis in ("gx", "gy", "gz")]


def fetch(copies):
    for copy in copies:
        copy.start()
    return copies


def arrive(copies):
    for copy in copies:
        copy.wait()


def lane_id():
    return lax.broadcasted_iota(jnp.int32, (SUB, LANES), 1)


def sub_id():
    return lax.broadcasted_iota(jnp.int32, (SUB, LANES), 0)


def gather(values, index, axis):
    return jnp.take_along_axis(values, index, axis=axis)


def swap_pairs(count):
    first = [(i, i ^ 1) for i in range(count)]
    second = [(i, (i + 1) % count if i % 2 else (i - 1) % count) for i in range(count)]
    return first, second


def swap(axis, first, second):
    count = lax.axis_size(axis)
    pairs_a, pairs_b = swap_pairs(count)
    got_a = lax.ppermute(first, axis, pairs_a)
    got_b = lax.ppermute(second, axis, pairs_b) if count > 2 else got_a
    return got_a, got_b


def pick_low(odd, got_a, got_b):
    return jnp.where(odd, got_a, got_b)


def pick_high(odd, got_a, got_b):
    return jnp.where(odd, got_b, got_a)


def extract(field, write, block_x, block_y, block_z):
    lanes = lane_id() // FOOT
    for quad in range(FOOT // 4):
        packed = None
        for inner in range(4):
            for part in range(FOOT // SUB):
                piece = field[FOOT * block_x + 4 * quad + inner, block_y * (FOOT // SUB) + part]
                spot = 2 * inner + part
                piece = pltpu.roll(piece, (FOOT * spot + LANES - FOOT * block_z) % LANES, 1)
                packed = piece if packed is None else jnp.where(lanes == spot, piece, packed)
        write(quad, packed)


def send_start_body(dims):
    group, slots, nbx, nby, nbz = dims

    def body(corner, owner, field, send, start, sem):
        copy = pltpu.make_async_copy(field, start, sem)
        copy.start()
        pos = place_of()
        lanes = lane_id()
        note = jnp.zeros((SUB, LANES), F32)
        blocks = []
        for slot in range(slots):
            block = (
                corner[0, 0, slot] // SIDE - pos[0] * nbx,
                corner[1, 0, slot] // SIDE - pos[1] * nby,
                corner[2, 0, slot] // SIDE - pos[2] * nbz,
            )
            blocks.append(block)
            for index, value in enumerate((owner[0, slot],) + block):
                note = jnp.where(lanes == 4 * slot + index, value.astype(F32), note)
        for target in range(group):
            send[target, 0:4] = jnp.zeros((4, SUB, LANES), F32)
            send[target, 4] = note
        copy.wait()
        for slot in range(slots):
            target = owner[0, slot]

            @pl.when(target < group)
            def _():
                def write(quad, packed):
                    send[target, quad] = packed

                extract(start, write, *blocks[slot])

    return body


def sides_body(ex):
    def body(start, shift, source, side_a, side_b, sems):
        pos = place_of()
        odd = pos[0] % 2
        copies = []
        for index, field in enumerate((start, shift, source)):
            for side, goal in enumerate((side_a, side_b)):
                high = 1 - odd if side == 0 else odd
                planes = field.at[pl.ds(high * (ex - WIDE), WIDE)]
                copies.append(pltpu.make_async_copy(planes, goal.at[index], sems.at[index, side]))
        for copy in copies:
            copy.start()
        for copy in copies:
            copy.wait()

    return body


def x_plane(field, got_a, got_b, odd, ex, xi):
    if xi < WIDE:
        return pick_low(odd, got_a[xi], got_b[xi])
    if xi < ex + WIDE:
        return field[xi - WIDE]
    return pick_high(odd, got_a[xi - ex - WIDE], got_b[xi - ex - WIDE])


def y_send_body(count, ex, nt):
    def body(*refs):
        fields, (xa, xb, ya, yb) = refs[:count], refs[count : count + 4]
        planes, sems = refs[count + 4 :]
        pos = place_of()
        odd_x = pos[0] % 2 == 1
        odd_y = pos[1] % 2 == 1
        copies = []
        for index in range(count):
            for side in range(2):
                tile = fields[index].at[:, side * (nt - 1)]
                copies.append(
                    pltpu.make_async_copy(tile, planes.at[index, side], sems.at[index, side])
                )
        fetch(copies)
        rows = sub_id()

        def pair(index, xi):
            found = []
            for at in (xi, xi + 1):
                if WIDE <= at < WIDE + ex:
                    found.append((planes[index, 0, at - WIDE], planes[index, 1, at - WIDE]))
                else:
                    plane = x_plane(None, xa.at[index], xb.at[index], odd_x, ex, at)
                    found.append((plane[0], plane[nt - 1]))
            (low, high), (low_next, high_next) = found
            low = jnp.where(rows < WIDE, low, pltpu.roll(low_next, WIDE, 0))
            high = jnp.where(rows < WIDE, pltpu.roll(high, WIDE, 0), high_next)
            ya[index, xi // 2] = jnp.where(odd_y, low, high)
            yb[index, xi // 2] = jnp.where(odd_y, high, low)

        edges = [*range(0, WIDE, 2), *range(WIDE + ex, 2 * WIDE + ex, 2)]
        for index in range(count):
            for xi in edges:
                pair(index, xi)
        arrive(copies)
        for index in range(count):
            for xi in range(WIDE, WIDE + ex, 2):
                pair(index, xi)

    return body


def seam_tile(ya, yb, odd_y, xi):
    low = pick_low(odd_y, ya[xi // 2], yb[xi // 2])
    high = pick_high(odd_y, ya[xi // 2], yb[xi // 2])
    if xi % 2 == 0:
        low = pltpu.roll(low, WIDE, 0)
    else:
        high = pltpu.roll(high, WIDE, 0)
    return jnp.where(sub_id() < WIDE, high, low)


def z_send_body(count, ex, nt):
    def body(*refs):
        raw, (xa, xb, ya, yb) = refs[:count], refs[count : count + 4]
        outs = refs[count + 4 : -2]
        fields, sems = refs[-2:]
        copies = [
            pltpu.make_async_copy(raw[index], fields.at[index], sems.at[index])
            for index in range(count)
        ]
        arrive(fetch(copies))
        pos = place_of()
        odd_x = pos[0] % 2 == 1
        odd_y = pos[1] % 2 == 1
        odd_z = pos[2] % 2
        lanes = lane_id() // WIDE
        per = LANES // WIDE
        for index in range(count):
            unit = 0
            packed = [None] * len(outs)
            total = (ex + 2 * WIDE) * (nt + 1)
            for xi in range(ex + 2 * WIDE):
                plane = x_plane(fields.at[index], xa.at[index], xb.at[index], odd_x, ex, xi)
                for tile in range(nt + 1):
                    if tile < nt:
                        value = plane[tile]
                    else:
                        value = seam_tile(ya.at[index], yb.at[index], odd_y, xi)
                    spot = unit % per
                    for which in range(len(outs)):
                        high = 1 - odd_z if which == 0 else odd_z
                        moved = pltpu.roll(value, (WIDE * spot + WIDE * high) % LANES, 1)
                        if spot == 0:
                            packed[which] = moved
                        else:
                            packed[which] = jnp.where(lanes == spot, moved, packed[which])
                        if spot == per - 1 or unit == total - 1:
                            outs[which][index, unit // per] = packed[which]
                    unit += 1

    return body


def halo_body(count, ex, nt, both, sizes):
    ny_rows = SUB * nt

    def inside_xy(pos, xi, tile):
        gx = pos[0] * ex + xi - WIDE
        ok = (gx >= 0) & (gx < sizes[0] * ex)
        row = sub_id()
        if tile < nt:
            return ok, None
        y = pos[1] * ny_rows + jnp.where(row < WIDE, ny_rows + row, row - SUB)
        return ok, (y >= 0) & (y < sizes[1] * ny_rows)

    def body(*refs):
        raw, (xa, xb, ya, yb) = refs[:count], refs[count : count + 4]
        rest = refs[count + 4 : -2]
        zs, outs = (rest[:2], rest[2:]) if both else (rest[:1], rest[1:])
        fields, sems = refs[-2:]
        copies = [
            pltpu.make_async_copy(raw[index], fields.at[index], sems.at[index])
            for index in range(count)
        ]
        arrive(fetch(copies))
        pos = place_of()
        odd_x = pos[0] % 2 == 1
        odd_y = pos[1] % 2 == 1
        odd_z = pos[2] % 2
        lanes = lane_id()
        per = LANES // WIDE
        has_high = pos[2] < sizes[2] - 1
        has_low = pos[2] > 0
        z_mask = ((lanes < WIDE) & has_high) | ((lanes >= LANES - WIDE) & has_low)
        unit = 0
        for xi in range(ex + 2 * WIDE):
            planes = [
                x_plane(fields.at[index], xa.at[index], xb.at[index], odd_x, ex, xi)
                for index in range(count)
            ]
            for tile in range(nt + 1):
                ok, rows = inside_xy(pos, xi, tile)
                if rows is None:
                    good = jnp.broadcast_to(ok, (SUB, LANES))
                else:
                    good = rows & ok
                spot = unit % per
                for index in range(count):
                    if tile < nt:
                        main = planes[index][tile]
                    else:
                        main = seam_tile(ya.at[index], yb.at[index], odd_y, xi)
                    parts = []
                    for which in range(len(zs)):
                        high = 1 - odd_z if which == 0 else odd_z
                        shift = (LANES - WIDE * spot + LANES - WIDE * (1 - high)) % LANES
                        parts.append(pltpu.roll(zs[which][index, unit // per], shift, 1))
                    if len(parts) == 1:
                        halo = parts[0]
                    else:
                        halo = jnp.where(
                            lanes < LANES // 2,
                            jnp.where(odd_z == 1, parts[1], parts[0]),
                            jnp.where(odd_z == 1, parts[0], parts[1]),
                        )
                    where_main = (xi, 0, slice(SUB * tile, SUB * tile + SUB))
                    where_halo = (xi, 1, slice(SUB * tile, SUB * tile + SUB))
                    if index == 0:
                        outs[0][where_main] = jnp.where(good, main, 0.0)
                        outs[0][where_halo] = jnp.where(good & z_mask, halo, 0.0)
                    elif index == 1:
                        outs[1][where_main] = jnp.where(good, OMEGA / (6.0 + main), 0.0)
                        diag = 6.0 + jnp.where(z_mask, halo, 0.0)
                        outs[1][where_halo] = jnp.where(good & z_mask, OMEGA / diag, 0.0)
                    else:
                        outs[2][where_main] = main
                        outs[2][where_halo] = jnp.where(z_mask, halo, 0.0)
                unit += 1

    return body


def around(value, ghost, masks):
    below, above, low_lanes, high_lanes, first, last = masks
    total = jnp.where(below, ghost, pltpu.roll(value, 1, 1))
    total = total + jnp.where(above, ghost, pltpu.roll(value, LANES - 1, 1))
    moved = pltpu.roll(value, SIDE, 1)
    moved = jnp.where(low_lanes, pltpu.roll(moved, 1, 0), moved)
    total = total + jnp.where(first, ghost, moved)
    moved = pltpu.roll(value, LANES - SIDE, 1)
    moved = jnp.where(high_lanes, pltpu.roll(moved, SUB - 1, 0), moved)
    return total + jnp.where(last, ghost, moved)


def fine_masks():
    lanes, rows = lane_id(), sub_id()
    low_lanes = lanes < SIDE
    high_lanes = lanes >= LANES - SIDE
    return (
        lanes % SIDE == 0,
        lanes % SIDE == SIDE - 1,
        low_lanes,
        high_lanes,
        low_lanes & (rows == 0),
        high_lanes & (rows == SUB - 1),
    )


def assign(rank, table, group, slots, found):
    count = jnp.int32(0)
    for home in range(group):
        for slot in range(slots):
            hit = table[home, COLS * slot] == rank

            @pl.when(hit)
            def _():
                found(count, home, slot)

            count = count + hit.astype(jnp.int32)
    return count


def unpack(packed, ghosts, slots):
    lanes, rows = lane_id(), sub_id()
    column = (lanes % SIDE) // 2
    row = (2 * rows + lanes // (LANES // 2)) % SUB
    upper = rows >= SUB // 2

    def box(index, carry):
        for quad in range(FOOT // 4):
            value = packed[index, quad]
            for inner in range(4):
                low = gather(value, 32 * inner + column, 1)
                high = gather(value, 32 * inner + FOOT + column, 1)
                plane = jnp.where(upper, gather(high, row, 0), gather(low, row, 0))
                ghosts[index, 4 * quad + inner] = plane
        return carry

    lax.fori_loop(0, slots, box, 0)


def prepare_body(slots):
    def body(source, shift, start, kept, rate, state, *scratch):
        ins, outs, sems = scratch[:3], scratch[3:6], scratch[6]
        arrive(
            fetch(
                [
                    pltpu.make_async_copy(raw, local, sems.at[index])
                    for index, (raw, local) in enumerate(zip((source, shift, start), ins))
                ]
            )
        )

        def load(index, carry):
            for x in range(SIDE):
                at = pl.ds(SIDE * x + index, SUB, stride=slots)
                outs[0][index, x] = ins[0][at, :]
                outs[1][index, x] = OMEGA / (6.0 + ins[1][at, :])
                outs[2][index, x] = ins[2][at, :]
            return carry

        lax.fori_loop(0, slots, load, 0)
        arrive(
            fetch(
                [
                    pltpu.make_async_copy(local, goal, sems.at[3 + index])
                    for index, (local, goal) in enumerate(zip(outs, (kept, rate, state)))
                ]
            )
        )

    return body


def fine_body(dims, first):
    group, slots, _, _, size_z = dims

    def body(*refs):
        if first:
            got, *stored = refs[:4]
            ret, state_out, ghosts_out, squares, table = refs[4:9]
            packed, other, state, ghosts, kept, rate, homes, moved, copied, counts, sems = refs[9:]
            old = (kept, rate, other)
        else:
            table, got, *stored = refs[:6]
            ret, state_out, ghosts_out, squares = refs[6:10]
            packed, other, state, ghosts, kept, rate, homes, moved, old_ghosts = refs[10:]
            old = (kept, rate, other, old_ghosts)
        loads = [
            pltpu.make_async_copy(source, goal, moved.at[index])
            for index, (source, goal) in enumerate(zip(stored, old))
        ]
        rank = lax.axis_index("gy") * size_z + lax.axis_index("gz")
        if first:
            for home in range(group):
                pltpu.make_async_copy(got.at[home, 4, 0], copied.at[home], sems.at[home]).start()
        fetch(loads)
        packed[...] = jnp.zeros(packed.shape, F32)
        if first:
            for home in range(group):
                pltpu.make_async_copy(got.at[home, 4, 0], copied.at[home], sems.at[home]).wait()
            for owner in range(group):
                counts[owner] = jnp.int32(0)
            for home in range(group):
                for slot in range(slots):
                    for index in range(4):
                        value = copied[home, 4 * slot + index].astype(jnp.int32)
                        table[home, COLS * slot + index] = value
                    owner = jnp.minimum(table[home, COLS * slot], group)
                    place = counts[owner]
                    table[home, COLS * slot + 4] = place
                    counts[owner] = place + 1

        def found(count, home, slot):
            packed[count] = got[home, 0:4]
            homes[count, 0] = jnp.int32(home)
            homes[count, 1] = table[home, COLS * slot + 2]
            homes[count, 2] = table[home, COLS * slot + 3]

        for slot in range(slots):
            homes[slot, 0] = jnp.int32(0)
            homes[slot, 1] = jnp.int32(0)
            homes[slot, 2] = jnp.int32(0)
        live = assign(rank, table, group, slots, found)
        unpack(packed, ghosts, slots)
        saves = [pltpu.make_async_copy(ghosts, ghosts_out, moved.at[4])]
        fetch(saves)
        arrive(loads)
        masks = fine_masks()
        lanes, rows = lane_id(), sub_id()

        def begin(index, carry):
            for x in range(SIDE):
                change = ghosts[index, x // 2] - old_ghosts[index, x // 2]
                other[index, x] = other[index, x] + change
            return carry

        if not first:
            lax.fori_loop(0, slots, begin, 0)

        def residual(buffer, index, x):
            value = buffer[index, x]
            ghost = ghosts[index, x // 2]
            near = around(value, ghost, masks)
            near = near + (buffer[index, x - 1] if x > 0 else ghost)
            near = near + (buffer[index, x + 1] if x < SIDE - 1 else ghost)
            return value, kept[index, x] + near

        buffers = [other, state, other, state]
        for sweep in range(FSWEEPS):
            here, there = buffers[sweep], buffers[sweep + 1]

            def step(index, carry):
                for x in range(SIDE):
                    value, rest = residual(here, index, x)
                    there[index, x] = (1.0 - OMEGA) * value + rate[index, x] * rest
                return carry

            lax.fori_loop(0, slots, step, 0)
        final = state
        saves.append(pltpu.make_async_copy(state, state_out, moved.at[5]))
        fetch(saves[1:])

        def remainder(index, x):
            value, rest = residual(final, index, x)
            return rest - (OMEGA / rate[index, x]) * value


        def finish(index, total):
            zone_y = jnp.where(homes[index, 1] == 0, 0, SUB - 2)
            zone_z = jnp.where(homes[index, 2] == 0, 0, FOOT - WIDE)
            column = (rows % 2) * (LANES // 2)
            take_all = column + 2 * (lanes % FOOT)
            take_z = column + 2 * (zone_z + lanes % WIDE)
            row_y = zone_y + (rows % 4) // 2
            row_low = rows // 2
            row_high = SUB // 2 + rows // 2
            mine = jnp.zeros((SUB, LANES), F32)
            y_slab = jnp.zeros((SUB, LANES), F32)
            z_slab = jnp.zeros((SUB, LANES), F32)
            whole = None
            for xp in range(FOOT):
                left = remainder(index, 2 * xp)
                mine = mine + left * left
                right = remainder(index, 2 * xp + 1)
                mine = mine + right * right
                both = left + right
                both = both + pltpu.roll(both, LANES - 1, 1)
                both = 0.125 * (both + pltpu.roll(both, LANES - SIDE, 1))
                piece = gather(gather(both, row_y, 0), take_all, 1)
                y_slab = jnp.where((lanes // FOOT == xp // 2) & (rows // 4 == xp % 2), piece, y_slab)
                for part in range(2):
                    picked = gather(both, row_high if part else row_low, 0)
                    piece = gather(picked, take_all, 1)
                    spot = 2 * (xp % 4) + part
                    whole = piece if spot == 0 else jnp.where(lanes // FOOT == spot, piece, whole)
                    piece = gather(picked, take_z, 1)
                    z_slab = jnp.where(lanes // WIDE == 2 * xp + part, piece, z_slab)
                if xp % 4 == 3:
                    packed[index, xp // 4] = whole
            home_z = homes[index, 0] % size_z
            for target in range(group):
                ret[target, 4 + index] = jnp.where(home_z == target % size_z, y_slab, z_slab)
            return total + jnp.where(index < live, mine, 0.0)

        squares[...] = lax.fori_loop(0, slots, finish, jnp.zeros((SUB, LANES), F32))
        for target in range(group):
            ret[target, 0:4] = jnp.zeros((4, SUB, LANES), F32)
        for index in range(slots):

            @pl.when(index < live)
            def _():
                ret[homes[index, 0], 0:4] = packed[index]

        arrive(saves)

    return body


def last_body(dims):
    group, slots, size_z = dims

    def body(table, got, old_state, old_ghosts, goal, packed, fresh, state, ghosts, result, sems):
        loads = [
            pltpu.make_async_copy(old_ghosts, ghosts, sems.at[0]),
            pltpu.make_async_copy(old_state, state, sems.at[1]),
        ]
        fetch(loads)
        rank = lax.axis_index("gy") * size_z + lax.axis_index("gz")
        packed[...] = jnp.zeros(packed.shape, F32)

        def found(count, home, slot):
            packed[count] = got[home, 0:4]

        live = assign(rank, table, group, slots, found)
        unpack(packed, fresh, slots)
        arrive(loads)

        def box(index, carry):
            for x in range(SIDE):
                value = state[index, x] + (fresh[index, x // 2] - ghosts[index, x // 2])
                value = jnp.where(index < live, value, 0.0)
                result[pl.ds(SIDE * x + index, SUB, stride=slots), :] = value
            return carry

        lax.fori_loop(0, slots, box, 0)
        arrive(fetch([pltpu.make_async_copy(result, goal, sems.at[2])]))

    return body


def norm_body(group):
    def body(got, total):
        result = got[0, 4]
        for peer in range(1, group):
            result = result + got[peer, 4]
        total[...] = result

    return body


def place_body(dims):
    ex, nt, group, slots, size_y, size_z, nby, nbz = dims
    tiles = FOOT // SUB

    def body(table, got, added, side_a, side_b):
        pos = place_of()
        odd = pos[0] % 2 == 1
        rank = pos[1] * size_z + pos[2]
        lanes, rows = lane_id(), sub_id()
        added[...] = jnp.zeros(added.shape, F32)

        def own(slot, carry):
            owner = table[rank, COLS * slot]

            @pl.when(owner < group)
            def _():
                base_x = FOOT * table[rank, COLS * slot + 1]
                base_y = tiles * table[rank, COLS * slot + 2]
                base_z = FOOT * table[rank, COLS * slot + 3]
                keep = (lanes >= base_z) & (lanes < base_z + FOOT)
                for quad in range(4):
                    value = got[owner, quad]
                    for inner in range(4):
                        for part in range(tiles):
                            spot = 2 * inner + part
                            moved = pltpu.roll(value, (base_z + LANES - FOOT * spot) % LANES, 1)
                            at = (base_x + 4 * quad + inner, 0, base_y + part)
                            added[at] = added[at] + jnp.where(keep, moved, 0.0)

            return carry

        lax.fori_loop(0, slots, own, 0)

        for dy in (-1, 0, 1):
            for dz in (-1, 0, 1):
                if dy == 0 and dz == 0:
                    continue
                home_y = pos[1] + dy
                home_z = pos[2] + dz
                exists = (home_y >= 0) & (home_y < size_y) & (home_z >= 0) & (home_z < size_z)
                home = jnp.where(exists, home_y * size_z + home_z, 0)

                def near(slot, carry):
                    owner = table[home, COLS * slot]
                    block_y = table[home, COLS * slot + 2]
                    block_z = table[home, COLS * slot + 3]
                    wanted = exists & (owner < group)
                    if dy != 0:
                        wanted = wanted & (block_y == (nby - 1 if dy < 0 else 0))
                    if dz != 0:
                        wanted = wanted & (block_z == (nbz - 1 if dz < 0 else 0))

                    @pl.when(wanted)
                    def _():
                        value = got[owner, 4 + table[home, COLS * slot + 4]]
                        base_x = FOOT * table[home, COLS * slot + 1]
                        goal = 0 if dy > 0 else 1
                        if dz == 0:
                            base_z = FOOT * block_z
                            keep = (lanes >= base_z) & (lanes < base_z + FOOT)
                            keep = keep & (rows // 4 == goal)
                            turned = pltpu.roll(value, 4, 0)
                            for x in range(FOOT):
                                use = value if x % 2 == goal else turned
                                shift = (base_z + LANES - FOOT * (x // 2)) % LANES
                                moved = pltpu.roll(use, shift, 1)
                                at = (base_x + x, 0, nt)
                                added[at] = added[at] + jnp.where(keep, moved, 0.0)
                        else:
                            where_z = 0 if dz > 0 else LANES - WIDE
                            keep = (lanes >= where_z) & (lanes < where_z + WIDE)
                            for x in range(FOOT):
                                for part in range(tiles):
                                    shift = (where_z + LANES - WIDE * (2 * x + part)) % LANES
                                    if dy == 0:
                                        moved = pltpu.roll(value, shift, 1)
                                        at = (base_x + x, 1, tiles * block_y + part)
                                        added[at] = added[at] + jnp.where(keep, moved, 0.0)
                                    elif part == (0 if dy > 0 else tiles - 1):
                                        moved = pltpu.roll(value, shift, 1)
                                        both = keep & (rows // 4 == goal)
                                        at = (base_x + x, 1, nt)
                                        added[at] = added[at] + jnp.where(both, moved, 0.0)

                    return carry

                lax.fori_loop(0, slots, near, 0)

        for low_side in (True, False):
            packed = None
            for index in range(WIDE - 1):
                plane = index if low_side else ex - (WIDE - 1) + index
                for tile in range(nt + 1):
                    spot = index * (nt + 1) + tile
                    moved = pltpu.roll(added[plane, 1, tile], WIDE + 2 * WIDE * spot, 1)
                    if spot == 0:
                        packed = moved
                    else:
                        packed = jnp.where(lanes // (2 * WIDE) == spot, moved, packed)
            units = (WIDE - 1) * (nt + 1)
            if low_side:
                low_packed = packed
            else:
                high_packed = packed
        for index in range(WIDE - 1):
            for tile in range(nt + 1):
                low = added[index, 0, tile]
                high = added[ex - (WIDE - 1) + index, 0, tile]
                spot = index * (nt + 1) + tile
                side_a[spot] = jnp.where(odd, low, high)
                side_b[spot] = jnp.where(odd, high, low)
        side_a[units] = jnp.where(odd, low_packed, high_packed)
        side_b[units] = jnp.where(odd, high_packed, low_packed)

    return body


def coarse_body(dims, more):
    ex, nt, group, slots, size_z = dims
    span = ex + 2 * WIDE
    rows_all = SUB * (nt + 1)

    def body(table, wide, rate, source, added, xa, xb, *refs):
        pos = place_of()
        sq_in, refs = refs[: 1 if more else 2], refs[1 if more else 2 :]
        if more:
            potential, send, squares, side_a, side_b = refs[:5]
        else:
            potential, send, squares = refs[:3]
        comp, one, two = refs[-3:]
        odd = pos[0] % 2 == 1
        rank = pos[1] * size_z + pos[2]
        lanes = lane_id()
        halo_lanes = (lanes < WIDE) | (lanes >= LANES - WIDE)
        units = (WIDE - 1) * (nt + 1)

        def fill(x, carry):
            for zone in range(2):
                for tile in range(nt + 1):
                    at = (WIDE + x, zone, pl.ds(SUB * tile, SUB))
                    comp[at] = source[at] + added[x, zone, tile]
            return carry

        lax.fori_loop(0, ex, fill, 0, unroll=True)
        low_tail = pick_low(odd, xa[units], xb[units])
        high_tail = pick_high(odd, xa[units], xb[units])
        for index in range(WIDE - 1):
            for tile in range(nt + 1):
                spot = index * (nt + 1) + tile
                shift = (LANES - WIDE - 2 * WIDE * spot) % LANES
                rows = slice(SUB * tile, SUB * tile + SUB)
                xi = 1 + index
                comp[xi, 0, rows] = source[xi, 0, rows] + pick_low(odd, xa[spot], xb[spot])
                tail = jnp.where(halo_lanes, pltpu.roll(low_tail, shift, 1), 0.0)
                comp[xi, 1, rows] = source[xi, 1, rows] + tail
                xi = WIDE + ex + index
                comp[xi, 0, rows] = source[xi, 0, rows] + pick_high(odd, xa[spot], xb[spot])
                tail = jnp.where(halo_lanes, pltpu.roll(high_tail, shift, 1), 0.0)
                comp[xi, 1, rows] = source[xi, 1, rows] + tail

        edge = lax.broadcasted_iota(jnp.int32, (rows_all, LANES), 1)

        def update(here, xi):
            main, halo = here[xi, 0], here[xi, 1]
            main_up, halo_up = pltpu.roll(main, 1, 1), pltpu.roll(halo, 1, 1)
            main_dn, halo_dn = pltpu.roll(main, LANES - 1, 1), pltpu.roll(halo, LANES - 1, 1)
            at_low, at_high = edge == 0, edge == LANES - 1
            result = []
            for zone, value in ((0, main), (1, halo)):
                if zone == 0:
                    near = jnp.where(at_low, halo_up, main_up) + jnp.where(at_high, halo_dn, main_dn)
                else:
                    near = jnp.where(at_low, main_up, halo_up) + jnp.where(at_high, main_dn, halo_dn)
                near = near + pltpu.roll(value, 1, 0) + pltpu.roll(value, rows_all - 1, 0)
                near = near + here[xi - 1, zone] + here[xi + 1, zone]
                rest = comp[xi, zone] + near
                result.append((value, rest))
            return result

        buffers = [wide, one, two, one]
        for sweep in range(CSWEEPS - 1):
            here, there = buffers[sweep], buffers[sweep + 1]

            def step(xi, carry):
                for zone, (value, rest) in enumerate(update(here, xi)):
                    there[xi, zone] = (1.0 - OMEGA) * value + rate[xi, zone] * rest
                return carry

            lax.fori_loop(1 + sweep, span - 1 - sweep, step, 0, unroll=True)
        here = buffers[CSWEEPS - 1]

        def step(x, total):
            value, rest = update(here, WIDE + x)[0]
            weight = rate[WIDE + x, 0]
            rest = rest - (OMEGA / weight) * value
            value = value + weight * rest
            for tile in range(nt):
                rows = slice(SUB * tile, SUB * tile + SUB)
                potential[x, tile] = value[rows]
                total = total + rest[rows] * rest[rows]
            return total

        total = lax.fori_loop(0, ex, step, sq_in[0][...], unroll=True)
        if more:
            squares[...] = total
        else:
            first_sum = jnp.sum(sq_in[1][...], axis=0, keepdims=True)
            second_sum = jnp.sum(total, axis=0, keepdims=True)
            squares[...] = jnp.where(sub_id() == 0, first_sum, second_sum)
        for target in range(group):
            send[target, 0:4] = jnp.zeros((4, SUB, LANES), F32)
            if not more:
                send[target, 4] = squares[...]
        for slot in range(slots):
            target = table[rank, COLS * slot]

            @pl.when(target < group)
            def _():
                def write(quad, packed):
                    send[target, quad] = packed

                block = [table[rank, COLS * slot + 1 + index] for index in range(3)]
                extract(potential, write, *block)

        if more:
            low = potential[0:WIDE]
            high = potential[ex - WIDE : ex]
            side_a[0] = jnp.where(odd, low, high)
            side_b[0] = jnp.where(odd, high, low)

    return body


def work(
    coarse_source,
    coarse_shift,
    coarse_start,
    fine_source,
    fine_shift,
    fine_start,
    box_corner,
    box_owner,
):
    ex, ey, ez = coarse_source.shape
    size_x, size_y, size_z = (lax.axis_size(axis) for axis in ("gx", "gy", "gz"))
    group = size_y * size_z
    slots, fine = fine_source.shape
    nbx, nby, nbz = ex // FOOT, ey // FOOT, ez // FOOT
    nt = ey // SUB
    assert ez == LANES and nby > 1 and fine == SIDE**3
    both = size_z > 2
    span = ex + 2 * WIDE
    sizes = (size_x, size_y, size_z)
    corner = jnp.transpose(box_corner, (2, 0, 1))

    def tiled(field):
        return field.reshape(ex, nt, SUB, LANES)

    def rows(field):
        count = fine // LANES
        return field.reshape(slots, count, LANES).transpose(1, 0, 2).reshape(count * slots, LANES)

    def exchange(value):
        return lax.all_to_all(value, GROUP_AXES, split_axis=0, concat_axis=0, tiled=True)

    start, shift, source = tiled(coarse_start), tiled(coarse_shift), tiled(coarse_source)
    f_source, f_shift, f_start = rows(fine_source), rows(fine_shift), rows(fine_start)

    def halos(fields, side_a, side_b, outs):
        count = len(fields)
        xa, xb = swap("gx", side_a, side_b)
        place = HBM if count > 1 else VMEM
        ins = [(place, field) for field in fields]
        ya, yb = call(
            y_send_body(count, ex, nt),
            ins + [(VMEM, xa), (VMEM, xb)],
            [(VMEM, out(count, span // 2, SUB, LANES))] * 2,
            [
                pltpu.VMEM((count, 2, ex, SUB, LANES), F32),
                pltpu.SemaphoreType.DMA((count, 2)),
            ],
        )
        ya, yb = swap("gy", ya, yb)
        units = -(-span * (nt + 1) // (LANES // WIDE))
        zs = call(
            z_send_body(count, ex, nt),
            ins + [(VMEM, value) for value in (xa, xb, ya, yb)],
            [(VMEM, out(count, units, SUB, LANES))] * (2 if both else 1),
            [
                pltpu.VMEM((count, ex, nt, SUB, LANES), F32),
                pltpu.SemaphoreType.DMA((count,)),
            ],
        )
        if both:
            zs = list(swap("gz", *zs))
        else:
            zs = [swap("gz", zs[0], zs[0])[0]]
        return call(
            halo_body(count, ex, nt, both, sizes),
            ins + [(VMEM, value) for value in (xa, xb, ya, yb, *zs)],
            [(VMEM, out(span, 2, SUB * (nt + 1), LANES))] * outs,
            [
                pltpu.VMEM((count, ex, nt, SUB, LANES), F32),
                pltpu.SemaphoreType.DMA((count,)),
            ],
        )

    (send,) = call(
        send_start_body((group, slots, nbx, nby, nbz)),
        [(SMEM, corner), (SMEM, box_owner), (HBM, start)],
        [(VMEM, out(group, 5, SUB, LANES))],
        [pltpu.VMEM((ex, nt, SUB, LANES), F32), pltpu.SemaphoreType.DMA],
    )
    got = exchange(send)
    fields = [start, shift, source]
    side_a, side_b = call(
        sides_body(ex),
        [(HBM, field) for field in fields],
        [(VMEM, out(3, WIDE, nt, SUB, LANES))] * 2,
        [pltpu.SemaphoreType.DMA((3, 2))],
    )
    wide, rate, source_wide = halos(fields, side_a, side_b, 3)

    box_shape = (slots, SIDE, SUB, LANES)
    flat = pltpu.VMEM((slots * fine // LANES, LANES), F32)
    whole = pltpu.VMEM(box_shape, F32)
    ghost = pltpu.VMEM((slots, FOOT, SUB, LANES), F32)
    packs = pltpu.VMEM((slots, 4, SUB, LANES), F32)
    kept, f_rate, state = call(
        prepare_body(slots),
        [(HBM, value) for value in (f_source, f_shift, f_start)],
        [(HBM, out(*box_shape))] * 3,
        [flat] * 3 + [whole] * 3 + [pltpu.SemaphoreType.DMA((6,))],
    )
    box_scratch = [packs, whole, whole, ghost, whole, whole]
    box_scratch += [pltpu.SMEM((slots, 3), jnp.int32), pltpu.SemaphoreType.DMA((6,))]
    box_outs = [
        (VMEM, out(group, 4 + slots, SUB, LANES)),
        (HBM, out(*box_shape)),
        (HBM, out(slots, FOOT, SUB, LANES)),
        (VMEM, out(SUB, LANES)),
    ]
    norms = []
    table = None
    for cycle in range(CYCLES):
        first = cycle == 0
        body = fine_body((group, slots, nby, nbz, size_z), first)
        if first:
            ret, state, ghosts, squares, table = call(
                body,
                [(VMEM, got)] + [(HBM, value) for value in (kept, f_rate, state)],
                box_outs + [(SMEM, out(group, COLS * slots, dtype=jnp.int32))],
                box_scratch
                + [
                    pltpu.SMEM((group, LANES), F32),
                    pltpu.SMEM((group + 1,), jnp.int32),
                    pltpu.SemaphoreType.DMA((group,)),
                ],
            )
        else:
            ret, state, ghosts, squares = call(
                body,
                [(SMEM, table), (VMEM, got)]
                + [(HBM, value) for value in (kept, f_rate, state, ghosts)],
                box_outs,
                box_scratch + [ghost],
            )
        back = exchange(ret)
        units = (WIDE - 1) * (nt + 1) + 1
        added, side_a, side_b = call(
            place_body((ex, nt, group, slots, size_y, size_z, nby, nbz)),
            [(SMEM, table), (VMEM, back)],
            [(VMEM, out(ex, 2, nt + 1, SUB, LANES))] + [(VMEM, out(units, SUB, LANES))] * 2,
        )
        xa, xb = swap("gx", side_a, side_b)
        more = cycle < CYCLES - 1
        wide_shape = (span, 2, SUB * (nt + 1), LANES)
        result = call(
            coarse_body((ex, nt, group, slots, size_z), more),
            [(SMEM, table)]
            + [(VMEM, v) for v in (wide, rate, source_wide, added, xa, xb, squares, *norms)],
            [
                (VMEM, out(ex, nt, SUB, LANES)),
                (VMEM, out(group, 4 if more else 5, SUB, LANES)),
                (VMEM, out(SUB, LANES)),
            ]
            + [(VMEM, out(1, WIDE, nt, SUB, LANES))] * (2 if more else 0),
            [pltpu.VMEM(wide_shape, F32)] * 3,
        )
        potential, send = result[:2]
        norms.append(result[2])
        got = exchange(send)
        if more:
            (wide,) = halos([potential], result[3], result[4], 1)
    (total,) = call(norm_body(group), [(VMEM, got)], [(VMEM, out(SUB, LANES))])
    (values,) = call(
        last_body((group, slots, size_z)),
        [(SMEM, table), (VMEM, got), (HBM, state), (HBM, ghosts)],
        [(HBM, out(slots * fine // LANES, LANES))],
        [packs, ghost, whole, ghost, flat, pltpu.SemaphoreType.DMA((3,))],
    )
    cells = float(ex * ey * ez * size_x * size_y * size_z)
    bit = 1
    while bit < size_x:
        pairs = [(i, i ^ bit) for i in range(size_x)]
        total = total + lax.ppermute(total, "gx", pairs)
        bit *= 2
    total = jnp.sum(total[:CYCLES], axis=1)
    values = values.reshape(fine // LANES, slots, LANES).transpose(1, 0, 2).reshape(slots, fine)
    return potential.reshape(ex, ey, ez), values, jnp.sqrt(total / cells)


def solution(mesh):
    in_specs = (
        P("gx", "gy", "gz"),
        P("gx", "gy", "gz"),
        P("gx", "gy", "gz"),
        P(("gx", "gy", "gz"), None),
        P(("gx", "gy", "gz"), None),
        P(("gx", "gy", "gz"), None),
        P(("gx", "gy", "gz"), None, None),
        P(("gx", "gy", "gz"), None),
    )
    out_specs = (P("gx", "gy", "gz"), P(("gx", "gy", "gz"), None), P())
    return jax.shard_map(work, mesh=mesh, in_specs=in_specs, out_specs=out_specs, check_vma=False)
```

```python
import jax
import jax.numpy as jnp
from jax import lax
from jax.experimental import pallas as pl
from jax.experimental.pallas import tpu as pltpu
from jax.sharding import PartitionSpec as P


FOOT = 16
CYCLES = 2
CSWEEPS = 4
FSWEEPS = 3
OMEGA = 0.8

SUB = 8
LANES = 128
SIDE = 2 * FOOT
WIDE = 4
COLS = 8
GROUP_AXES = ("gy", "gz")

VMEM = pl.BlockSpec(memory_space=pltpu.VMEM)
SMEM = pl.BlockSpec(memory_space=pltpu.SMEM)
HBM = pl.BlockSpec(memory_space=pltpu.HBM)
F32 = jnp.float32


def out(*shape, dtype=F32):
    return jax.ShapeDtypeStruct(shape, dtype)


def call(body, ins, outs, scratch=()):
    values = [
        pltpu.with_memory_space_constraint(value, pltpu.HBM) if spec is HBM else value
        for spec, value in ins
    ]
    shapes = [pltpu.HBM(shape.shape, shape.dtype) if spec is HBM else shape for spec, shape in outs]
    return pl.pallas_call(
        body,
        in_specs=[spec for spec, _ in ins],
        out_specs=[spec for spec, _ in outs],
        out_shape=shapes,
        scratch_shapes=list(scratch),
        compiler_params=pltpu.CompilerParams(vmem_limit_bytes=16 << 20),
    )(*values)


def place_of():
    return [lax.axis_index(axis) for axis in ("gx", "gy", "gz")]


def fetch(copies):
    for copy in copies:
        copy.start()
    return copies


def arrive(copies):
    for copy in copies:
        copy.wait()


def lane_id():
    return lax.broadcasted_iota(jnp.int32, (SUB, LANES), 1)


def sub_id():
    return lax.broadcasted_iota(jnp.int32, (SUB, LANES), 0)


def gather(values, index, axis):
    return jnp.take_along_axis(values, index, axis=axis)


def swap_pairs(count):
    first = [(i, i ^ 1) for i in range(count)]
    second = [(i, (i + 1) % count if i % 2 else (i - 1) % count) for i in range(count)]
    return first, second


def swap(axis, first, second):
    count = lax.axis_size(axis)
    pairs_a, pairs_b = swap_pairs(count)
    got_a = lax.ppermute(first, axis, pairs_a)
    got_b = lax.ppermute(second, axis, pairs_b) if count > 2 else got_a
    return got_a, got_b


def pick_low(odd, got_a, got_b):
    return jnp.where(odd, got_a, got_b)


def pick_high(odd, got_a, got_b):
    return jnp.where(odd, got_b, got_a)


def extract(field, write, block_x, block_y, block_z):
    lanes = lane_id() // FOOT
    for quad in range(FOOT // 4):
        packed = None
        for inner in range(4):
            for part in range(FOOT // SUB):
                piece = field[FOOT * block_x + 4 * quad + inner, block_y * (FOOT // SUB) + part]
                spot = 2 * inner + part
                piece = pltpu.roll(piece, (FOOT * spot + LANES - FOOT * block_z) % LANES, 1)
                packed = piece if packed is None else jnp.where(lanes == spot, piece, packed)
        write(quad, packed)


def send_start_body(dims):
    ex, group, slots, nbx, nby, nbz = dims

    def body(
        corner_in, owner_in, field, shift, source, send, side_a, side_b, start, corner, owner, sem, sems
    ):
        small = [
            pltpu.make_async_copy(corner_in, corner, sem.at[1]),
            pltpu.make_async_copy(owner_in, owner, sem.at[2]),
        ]
        fetch(small)
        copy = pltpu.make_async_copy(field, start, sem.at[0])
        copy.start()
        odd = lax.axis_index("gx") % 2
        sides = []
        for index, raw in enumerate((field, shift, source)):
            for side, goal in enumerate((side_a, side_b)):
                high = 1 - odd if side == 0 else odd
                planes = raw.at[pl.ds(high * (ex - WIDE), WIDE)]
                sides.append(pltpu.make_async_copy(planes, goal.at[index], sems.at[index, side]))
        fetch(sides)
        arrive(small)
        pos = place_of()
        lanes = lane_id()
        note = jnp.zeros((SUB, LANES), F32)
        blocks = []
        for slot in range(slots):
            block = (
                corner[0, 0, slot] // SIDE - pos[0] * nbx,
                corner[1, 0, slot] // SIDE - pos[1] * nby,
                corner[2, 0, slot] // SIDE - pos[2] * nbz,
            )
            blocks.append(block)
            for index, value in enumerate((owner[0, slot],) + block):
                note = jnp.where(lanes == 4 * slot + index, value.astype(F32), note)
        for target in range(group):
            send[target, 0:4] = jnp.zeros((4, SUB, LANES), F32)
            send[target, 4] = note
        copy.wait()
        for slot in range(slots):
            target = owner[0, slot]

            @pl.when(target < group)
            def _():
                def write(quad, packed):
                    send[target, quad] = packed

                extract(start, write, *blocks[slot])

        arrive(sides)

    return body


def x_plane(field, got_a, got_b, odd, ex, xi):
    if xi < WIDE:
        return pick_low(odd, got_a[xi], got_b[xi])
    if xi < ex + WIDE:
        return field[xi - WIDE]
    return pick_high(odd, got_a[xi - ex - WIDE], got_b[xi - ex - WIDE])


def y_send_body(count, ex, nt):
    def body(*refs):
        fields, (xa, xb, ya, yb) = refs[:count], refs[count : count + 4]
        planes, sems = refs[count + 4 :]
        pos = place_of()
        odd_x = pos[0] % 2 == 1
        odd_y = pos[1] % 2 == 1
        copies = []
        for index in range(count):
            for side in range(2):
                tile = fields[index].at[:, side * (nt - 1)]
                copies.append(
                    pltpu.make_async_copy(tile, planes.at[index, side], sems.at[index, side])
                )
        fetch(copies)
        rows = sub_id()

        def pair(index, xi):
            found = []
            for at in (xi, xi + 1):
                if WIDE <= at < WIDE + ex:
                    found.append((planes[index, 0, at - WIDE], planes[index, 1, at - WIDE]))
                else:
                    plane = x_plane(None, xa.at[index], xb.at[index], odd_x, ex, at)
                    found.append((plane[0], plane[nt - 1]))
            (low, high), (low_next, high_next) = found
            low = jnp.where(rows < WIDE, low, pltpu.roll(low_next, WIDE, 0))
            high = jnp.where(rows < WIDE, pltpu.roll(high, WIDE, 0), high_next)
            ya[index, xi // 2] = jnp.where(odd_y, low, high)
            yb[index, xi // 2] = jnp.where(odd_y, high, low)

        edges = [*range(0, WIDE, 2), *range(WIDE + ex, 2 * WIDE + ex, 2)]
        for index in range(count):
            for xi in edges:
                pair(index, xi)
        arrive(copies)
        for index in range(count):
            for xi in range(WIDE, WIDE + ex, 2):
                pair(index, xi)

    return body


def seam_tile(ya, yb, odd_y, xi):
    low = pick_low(odd_y, ya[xi // 2], yb[xi // 2])
    high = pick_high(odd_y, ya[xi // 2], yb[xi // 2])
    if xi % 2 == 0:
        low = pltpu.roll(low, WIDE, 0)
    else:
        high = pltpu.roll(high, WIDE, 0)
    return jnp.where(sub_id() < WIDE, high, low)


def z_send_body(count, ex, nt):
    def body(*refs):
        raw, (xa, xb, ya, yb) = refs[:count], refs[count : count + 4]
        outs = refs[count + 4 : -2]
        fields, sems = refs[-2:]
        copies = [
            pltpu.make_async_copy(raw[index], fields.at[index], sems.at[index])
            for index in range(count)
        ]
        arrive(fetch(copies))
        pos = place_of()
        odd_x = pos[0] % 2 == 1
        odd_y = pos[1] % 2 == 1
        odd_z = pos[2] % 2
        lanes = lane_id() // WIDE
        per = LANES // WIDE
        for index in range(count):
            unit = 0
            packed = [None] * len(outs)
            total = (ex + 2 * WIDE) * (nt + 1)
            for xi in range(ex + 2 * WIDE):
                plane = x_plane(fields.at[index], xa.at[index], xb.at[index], odd_x, ex, xi)
                for tile in range(nt + 1):
                    if tile < nt:
                        value = plane[tile]
                    else:
                        value = seam_tile(ya.at[index], yb.at[index], odd_y, xi)
                    spot = unit % per
                    for which in range(len(outs)):
                        high = 1 - odd_z if which == 0 else odd_z
                        moved = pltpu.roll(value, (WIDE * spot + WIDE * high) % LANES, 1)
                        if spot == 0:
                            packed[which] = moved
                        else:
                            packed[which] = jnp.where(lanes == spot, moved, packed[which])
                        if spot == per - 1 or unit == total - 1:
                            outs[which][index, unit // per] = packed[which]
                    unit += 1

    return body


def halo_body(count, ex, nt, both, sizes):
    ny_rows = SUB * nt

    def inside_xy(pos, xi, tile):
        gx = pos[0] * ex + xi - WIDE
        ok = (gx >= 0) & (gx < sizes[0] * ex)
        row = sub_id()
        if tile < nt:
            return ok, None
        y = pos[1] * ny_rows + jnp.where(row < WIDE, ny_rows + row, row - SUB)
        return ok, (y >= 0) & (y < sizes[1] * ny_rows)

    def body(*refs):
        raw, (xa, xb, ya, yb) = refs[:count], refs[count : count + 4]
        rest = refs[count + 4 : -2]
        zs, outs = (rest[:2], rest[2:]) if both else (rest[:1], rest[1:])
        fields, sems = refs[-2:]
        copies = [
            pltpu.make_async_copy(raw[index], fields.at[index], sems.at[index])
            for index in range(count)
        ]
        arrive(fetch(copies))
        pos = place_of()
        odd_x = pos[0] % 2 == 1
        odd_y = pos[1] % 2 == 1
        odd_z = pos[2] % 2
        lanes = lane_id()
        per = LANES // WIDE
        has_high = pos[2] < sizes[2] - 1
        has_low = pos[2] > 0
        z_mask = ((lanes < WIDE) & has_high) | ((lanes >= LANES - WIDE) & has_low)
        unit = 0
        for xi in range(ex + 2 * WIDE):
            planes = [
                x_plane(fields.at[index], xa.at[index], xb.at[index], odd_x, ex, xi)
                for index in range(count)
            ]
            for tile in range(nt + 1):
                ok, rows = inside_xy(pos, xi, tile)
                if rows is None:
                    good = jnp.broadcast_to(ok, (SUB, LANES))
                else:
                    good = rows & ok
                spot = unit % per
                for index in range(count):
                    if tile < nt:
                        main = planes[index][tile]
                    else:
                        main = seam_tile(ya.at[index], yb.at[index], odd_y, xi)
                    parts = []
                    for which in range(len(zs)):
                        high = 1 - odd_z if which == 0 else odd_z
                        shift = (LANES - WIDE * spot + LANES - WIDE * (1 - high)) % LANES
                        parts.append(pltpu.roll(zs[which][index, unit // per], shift, 1))
                    if len(parts) == 1:
                        halo = parts[0]
                    else:
                        halo = jnp.where(
                            lanes < LANES // 2,
                            jnp.where(odd_z == 1, parts[1], parts[0]),
                            jnp.where(odd_z == 1, parts[0], parts[1]),
                        )
                    where_main = (xi, 0, slice(SUB * tile, SUB * tile + SUB))
                    where_halo = (xi, 1, slice(SUB * tile, SUB * tile + SUB))
                    if index == 0:
                        outs[0][where_main] = jnp.where(good, main, 0.0)
                        outs[0][where_halo] = jnp.where(good & z_mask, halo, 0.0)
                    elif index == 1:
                        outs[1][where_main] = jnp.where(good, OMEGA / (6.0 + main), 0.0)
                        diag = 6.0 + jnp.where(z_mask, halo, 0.0)
                        outs[1][where_halo] = jnp.where(good & z_mask, OMEGA / diag, 0.0)
                    else:
                        outs[2][where_main] = main
                        outs[2][where_halo] = jnp.where(z_mask, halo, 0.0)
                unit += 1

    return body


def around(value, ghost, masks):
    below, above, low_lanes, high_lanes, first, last = masks
    total = jnp.where(below, ghost, pltpu.roll(value, 1, 1))
    total = total + jnp.where(above, ghost, pltpu.roll(value, LANES - 1, 1))
    moved = pltpu.roll(value, SIDE, 1)
    moved = jnp.where(low_lanes, pltpu.roll(moved, 1, 0), moved)
    total = total + jnp.where(first, ghost, moved)
    moved = pltpu.roll(value, LANES - SIDE, 1)
    moved = jnp.where(high_lanes, pltpu.roll(moved, SUB - 1, 0), moved)
    return total + jnp.where(last, ghost, moved)


def fine_masks():
    lanes, rows = lane_id(), sub_id()
    low_lanes = lanes < SIDE
    high_lanes = lanes >= LANES - SIDE
    return (
        lanes % SIDE == 0,
        lanes % SIDE == SIDE - 1,
        low_lanes,
        high_lanes,
        low_lanes & (rows == 0),
        high_lanes & (rows == SUB - 1),
    )


def assign(rank, table, group, slots, found):
    count = jnp.int32(0)
    for home in range(group):
        for slot in range(slots):
            hit = table[home, COLS * slot] == rank

            @pl.when(hit)
            def _():
                found(count, home, slot)

            count = count + hit.astype(jnp.int32)
    return count


def unpack(packed, ghosts, slots):
    lanes, rows = lane_id(), sub_id()
    column = (lanes % SIDE) // 2
    row = (2 * rows + lanes // (LANES // 2)) % SUB
    upper = rows >= SUB // 2

    def box(index, carry):
        for quad in range(FOOT // 4):
            value = packed[index, quad]
            for inner in range(4):
                low = gather(value, 32 * inner + column, 1)
                high = gather(value, 32 * inner + FOOT + column, 1)
                plane = jnp.where(upper, gather(high, row, 0), gather(low, row, 0))
                ghosts[index, 4 * quad + inner] = plane
        return carry

    lax.fori_loop(0, slots, box, 0)


def fine_body(dims, first):
    group, slots, _, _, size_z = dims

    def body(*refs):
        if first:
            got, *stored = refs[:4]
            ret, state_out, squares, table, kept_out, rate_out = refs[4:10]
            packed, other, state, ghosts, kept, rate, homes, moved, copied, counts, sems = refs[10:21]
            old = refs[21:]
        else:
            table, got, *stored = refs[:5]
            ret, state_out, squares = refs[5:8]
            packed, other, state, ghosts, kept, rate, homes, moved = refs[8:]
            old = (other, kept, rate)
        loads = [
            pltpu.make_async_copy(source, goal, moved.at[index])
            for index, (source, goal) in enumerate(zip(stored, old))
        ]
        rank = lax.axis_index("gy") * size_z + lax.axis_index("gz")
        if first:
            for home in range(group):
                pltpu.make_async_copy(got.at[home, 4, 0], copied.at[home], sems.at[home]).start()
        fetch(loads)
        packed[...] = jnp.zeros(packed.shape, F32)
        if first:
            for home in range(group):
                pltpu.make_async_copy(got.at[home, 4, 0], copied.at[home], sems.at[home]).wait()
            for owner in range(group):
                counts[owner] = jnp.int32(0)
            for home in range(group):
                for slot in range(slots):
                    for index in range(4):
                        value = copied[home, 4 * slot + index].astype(jnp.int32)
                        table[home, COLS * slot + index] = value
                    owner = jnp.minimum(table[home, COLS * slot], group)
                    place = counts[owner]
                    table[home, COLS * slot + 4] = place
                    counts[owner] = place + 1

        def found(count, home, slot):
            packed[count] = got[home, 0:4]
            homes[count, 0] = jnp.int32(home)
            homes[count, 1] = table[home, COLS * slot + 2]
            homes[count, 2] = table[home, COLS * slot + 3]

        for slot in range(slots):
            homes[slot, 0] = jnp.int32(0)
            homes[slot, 1] = jnp.int32(0)
            homes[slot, 2] = jnp.int32(0)
        live = assign(rank, table, group, slots, found)
        unpack(packed, ghosts, slots)
        saves = []
        arrive(loads if first else loads[:1])
        masks = fine_masks()
        lanes, rows = lane_id(), sub_id()

        def convert(index, carry):
            for x in range(SIDE):
                at = pl.ds(SIDE * x + index, SUB, stride=slots)
                kept[index, x] = old[0][at, :]
                rate[index, x] = OMEGA / (6.0 + old[1][at, :])
                other[index, x] = old[2][at, :]
            return carry

        if first:
            lax.fori_loop(0, slots, convert, 0)
            saves.append(pltpu.make_async_copy(kept, kept_out, moved.at[6]))
            saves.append(pltpu.make_async_copy(rate, rate_out, moved.at[7]))
            fetch(saves)

        def begin(index, carry):
            for x in range(SIDE):
                other[index, x] = other[index, x] + ghosts[index, x // 2]
            return carry

        if not first:
            lax.fori_loop(0, slots, begin, 0)
            arrive(loads[1:])

        def residual(buffer, index, x):
            value = buffer[index, x]
            ghost = ghosts[index, x // 2]
            near = around(value, ghost, masks)
            near = near + (buffer[index, x - 1] if x > 0 else ghost)
            near = near + (buffer[index, x + 1] if x < SIDE - 1 else ghost)
            return value, kept[index, x] + near

        buffers = [other, state, other, state]
        for sweep in range(FSWEEPS):
            here, there = buffers[sweep], buffers[sweep + 1]

            def step(index, carry):
                for x in range(SIDE):
                    value, rest = residual(here, index, x)
                    there[index, x] = (1.0 - OMEGA) * value + rate[index, x] * rest
                return carry

            lax.fori_loop(0, slots, step, 0)
        final = state

        def save(index):
            return pltpu.make_async_copy(other.at[index], state_out.at[index], moved.at[index])

        def remainder(index, x):
            value, rest = residual(final, index, x)
            other[index, x] = value - ghosts[index, x // 2]
            return rest - (OMEGA / rate[index, x]) * value


        def finish(index, total):
            zone_y = jnp.where(homes[index, 1] == 0, 0, SUB - 2)
            zone_z = jnp.where(homes[index, 2] == 0, 0, FOOT - WIDE)
            column = (rows % 2) * (LANES // 2)
            take_all = column + 2 * (lanes % FOOT)
            take_z = column + 2 * (zone_z + lanes % WIDE)
            row_y = zone_y + (rows % 4) // 2
            row_low = rows // 2
            row_high = SUB // 2 + rows // 2
            mine = jnp.zeros((SUB, LANES), F32)
            y_slab = jnp.zeros((SUB, LANES), F32)
            z_slab = jnp.zeros((SUB, LANES), F32)
            whole = None
            for xp in range(FOOT):
                left = remainder(index, 2 * xp)
                mine = mine + left * left
                right = remainder(index, 2 * xp + 1)
                mine = mine + right * right
                both = left + right
                both = both + pltpu.roll(both, LANES - 1, 1)
                both = 0.125 * (both + pltpu.roll(both, LANES - SIDE, 1))
                piece = gather(gather(both, row_y, 0), take_all, 1)
                y_slab = jnp.where((lanes // FOOT == xp // 2) & (rows // 4 == xp % 2), piece, y_slab)
                for part in range(2):
                    picked = gather(both, row_high if part else row_low, 0)
                    piece = gather(picked, take_all, 1)
                    spot = 2 * (xp % 4) + part
                    whole = piece if spot == 0 else jnp.where(lanes // FOOT == spot, piece, whole)
                    piece = gather(picked, take_z, 1)
                    z_slab = jnp.where(lanes // WIDE == 2 * xp + part, piece, z_slab)
                if xp % 4 == 3:
                    packed[index, xp // 4] = whole
            save(index).start()
            home_z = homes[index, 0] % size_z
            for target in range(group):
                ret[target, 4 + index] = jnp.where(home_z == target % size_z, y_slab, z_slab)
            return total + jnp.where(index < live, mine, 0.0)

        squares[...] = lax.fori_loop(0, slots, finish, jnp.zeros((SUB, LANES), F32))
        for target in range(group):
            ret[target, 0:4] = jnp.zeros((4, SUB, LANES), F32)
        for index in range(slots):

            @pl.when(index < live)
            def _():
                ret[homes[index, 0], 0:4] = packed[index]

        arrive(saves)
        arrive([save(index) for index in range(slots)])

    return body


def last_body(dims):
    group, slots, size_z = dims

    def body(table, got, old_state, goal, packed, fresh, state, result, sems):
        loads = [pltpu.make_async_copy(old_state, state, sems.at[0])]
        fetch(loads)
        rank = lax.axis_index("gy") * size_z + lax.axis_index("gz")
        packed[...] = jnp.zeros(packed.shape, F32)

        def found(count, home, slot):
            packed[count] = got[home, 0:4]

        live = assign(rank, table, group, slots, found)
        unpack(packed, fresh, slots)
        arrive(loads)

        def box(index, carry):
            for x in range(SIDE):
                value = state[index, x] + fresh[index, x // 2]
                value = jnp.where(index < live, value, 0.0)
                result[pl.ds(SIDE * x + index, SUB, stride=slots), :] = value
            return carry

        lax.fori_loop(0, slots, box, 0)
        arrive(fetch([pltpu.make_async_copy(result, goal, sems.at[1])]))

    return body


def norm_body(group):
    def body(got, total):
        result = got[0, 4]
        for peer in range(1, group):
            result = result + got[peer, 4]
        total[...] = result

    return body


def place_body(dims):
    ex, nt, group, slots, size_y, size_z, nby, nbz = dims
    tiles = FOOT // SUB

    def body(table, got, added, side_a, side_b):
        pos = place_of()
        odd = pos[0] % 2 == 1
        rank = pos[1] * size_z + pos[2]
        lanes, rows = lane_id(), sub_id()
        added[...] = jnp.zeros(added.shape, F32)

        def own(slot, carry):
            owner = table[rank, COLS * slot]

            @pl.when(owner < group)
            def _():
                base_x = FOOT * table[rank, COLS * slot + 1]
                base_y = tiles * table[rank, COLS * slot + 2]
                base_z = FOOT * table[rank, COLS * slot + 3]
                keep = (lanes >= base_z) & (lanes < base_z + FOOT)
                for quad in range(4):
                    value = got[owner, quad]
                    for inner in range(4):
                        for part in range(tiles):
                            spot = 2 * inner + part
                            moved = pltpu.roll(value, (base_z + LANES - FOOT * spot) % LANES, 1)
                            at = (base_x + 4 * quad + inner, 0, base_y + part)
                            added[at] = added[at] + jnp.where(keep, moved, 0.0)

            return carry

        lax.fori_loop(0, slots, own, 0)

        for dy in (-1, 0, 1):
            for dz in (-1, 0, 1):
                if dy == 0 and dz == 0:
                    continue
                home_y = pos[1] + dy
                home_z = pos[2] + dz
                exists = (home_y >= 0) & (home_y < size_y) & (home_z >= 0) & (home_z < size_z)
                home = jnp.where(exists, home_y * size_z + home_z, 0)

                def near(slot, carry):
                    owner = table[home, COLS * slot]
                    block_y = table[home, COLS * slot + 2]
                    block_z = table[home, COLS * slot + 3]
                    wanted = exists & (owner < group)
                    if dy != 0:
                        wanted = wanted & (block_y == (nby - 1 if dy < 0 else 0))
                    if dz != 0:
                        wanted = wanted & (block_z == (nbz - 1 if dz < 0 else 0))

                    @pl.when(wanted)
                    def _():
                        value = got[owner, 4 + table[home, COLS * slot + 4]]
                        base_x = FOOT * table[home, COLS * slot + 1]
                        goal = 0 if dy > 0 else 1
                        if dz == 0:
                            base_z = FOOT * block_z
                            keep = (lanes >= base_z) & (lanes < base_z + FOOT)
                            keep = keep & (rows // 4 == goal)
                            turned = pltpu.roll(value, 4, 0)
                            for x in range(FOOT):
                                use = value if x % 2 == goal else turned
                                shift = (base_z + LANES - FOOT * (x // 2)) % LANES
                                moved = pltpu.roll(use, shift, 1)
                                at = (base_x + x, 0, nt)
                                added[at] = added[at] + jnp.where(keep, moved, 0.0)
                        else:
                            where_z = 0 if dz > 0 else LANES - WIDE
                            keep = (lanes >= where_z) & (lanes < where_z + WIDE)
                            for x in range(FOOT):
                                for part in range(tiles):
                                    shift = (where_z + LANES - WIDE * (2 * x + part)) % LANES
                                    if dy == 0:
                                        moved = pltpu.roll(value, shift, 1)
                                        at = (base_x + x, 1, tiles * block_y + part)
                                        added[at] = added[at] + jnp.where(keep, moved, 0.0)
                                    elif part == (0 if dy > 0 else tiles - 1):
                                        moved = pltpu.roll(value, shift, 1)
                                        both = keep & (rows // 4 == goal)
                                        at = (base_x + x, 1, nt)
                                        added[at] = added[at] + jnp.where(both, moved, 0.0)

                    return carry

                lax.fori_loop(0, slots, near, 0)

        for low_side in (True, False):
            packed = None
            for index in range(WIDE - 1):
                plane = index if low_side else ex - (WIDE - 1) + index
                for tile in range(nt + 1):
                    spot = index * (nt + 1) + tile
                    moved = pltpu.roll(added[plane, 1, tile], WIDE + 2 * WIDE * spot, 1)
                    if spot == 0:
                        packed = moved
                    else:
                        packed = jnp.where(lanes // (2 * WIDE) == spot, moved, packed)
            units = (WIDE - 1) * (nt + 1)
            if low_side:
                low_packed = packed
            else:
                high_packed = packed
        for index in range(WIDE - 1):
            for tile in range(nt + 1):
                low = added[index, 0, tile]
                high = added[ex - (WIDE - 1) + index, 0, tile]
                spot = index * (nt + 1) + tile
                side_a[spot] = jnp.where(odd, low, high)
                side_b[spot] = jnp.where(odd, high, low)
        side_a[units] = jnp.where(odd, low_packed, high_packed)
        side_b[units] = jnp.where(odd, high_packed, low_packed)

    return body


def coarse_body(dims, more):
    ex, nt, group, slots, size_z = dims
    span = ex + 2 * WIDE
    rows_all = SUB * (nt + 1)

    def body(table, wide, rate, source, added, xa, xb, *refs):
        pos = place_of()
        sq_in, refs = refs[: 1 if more else 2], refs[1 if more else 2 :]
        if more:
            potential, send, squares, side_a, side_b = refs[:5]
        else:
            potential, send, squares = refs[:3]
        comp, one, two = refs[-3:]
        odd = pos[0] % 2 == 1
        rank = pos[1] * size_z + pos[2]
        lanes = lane_id()
        halo_lanes = (lanes < WIDE) | (lanes >= LANES - WIDE)
        units = (WIDE - 1) * (nt + 1)

        def fill(x, carry):
            for zone in range(2):
                for tile in range(nt + 1):
                    at = (WIDE + x, zone, pl.ds(SUB * tile, SUB))
                    comp[at] = source[at] + added[x, zone, tile]
            return carry

        lax.fori_loop(0, ex, fill, 0, unroll=True)
        low_tail = pick_low(odd, xa[units], xb[units])
        high_tail = pick_high(odd, xa[units], xb[units])
        for index in range(WIDE - 1):
            for tile in range(nt + 1):
                spot = index * (nt + 1) + tile
                shift = (LANES - WIDE - 2 * WIDE * spot) % LANES
                rows = slice(SUB * tile, SUB * tile + SUB)
                xi = 1 + index
                comp[xi, 0, rows] = source[xi, 0, rows] + pick_low(odd, xa[spot], xb[spot])
                tail = jnp.where(halo_lanes, pltpu.roll(low_tail, shift, 1), 0.0)
                comp[xi, 1, rows] = source[xi, 1, rows] + tail
                xi = WIDE + ex + index
                comp[xi, 0, rows] = source[xi, 0, rows] + pick_high(odd, xa[spot], xb[spot])
                tail = jnp.where(halo_lanes, pltpu.roll(high_tail, shift, 1), 0.0)
                comp[xi, 1, rows] = source[xi, 1, rows] + tail

        edge = lax.broadcasted_iota(jnp.int32, (rows_all, LANES), 1)

        def update(here, xi):
            main, halo = here[xi, 0], here[xi, 1]
            main_up, halo_up = pltpu.roll(main, 1, 1), pltpu.roll(halo, 1, 1)
            main_dn, halo_dn = pltpu.roll(main, LANES - 1, 1), pltpu.roll(halo, LANES - 1, 1)
            at_low, at_high = edge == 0, edge == LANES - 1
            result = []
            for zone, value in ((0, main), (1, halo)):
                if zone == 0:
                    near = jnp.where(at_low, halo_up, main_up) + jnp.where(at_high, halo_dn, main_dn)
                else:
                    near = jnp.where(at_low, main_up, halo_up) + jnp.where(at_high, main_dn, halo_dn)
                near = near + pltpu.roll(value, 1, 0) + pltpu.roll(value, rows_all - 1, 0)
                near = near + here[xi - 1, zone] + here[xi + 1, zone]
                rest = comp[xi, zone] + near
                result.append((value, rest))
            return result

        buffers = [wide, one, two, one]
        for sweep in range(CSWEEPS - 1):
            here, there = buffers[sweep], buffers[sweep + 1]

            def step(xi, carry):
                for zone, (value, rest) in enumerate(update(here, xi)):
                    there[xi, zone] = (1.0 - OMEGA) * value + rate[xi, zone] * rest
                return carry

            lax.fori_loop(1 + sweep, span - 1 - sweep, step, 0, unroll=True)
        here = buffers[CSWEEPS - 1]

        def step(x, total):
            value, rest = update(here, WIDE + x)[0]
            weight = rate[WIDE + x, 0]
            rest = rest - (OMEGA / weight) * value
            value = value + weight * rest
            for tile in range(nt):
                rows = slice(SUB * tile, SUB * tile + SUB)
                potential[x, tile] = value[rows]
                total = total + rest[rows] * rest[rows]
            return total

        total = lax.fori_loop(0, ex, step, sq_in[0][...], unroll=True)
        if more:
            squares[...] = total
        else:
            first_sum = jnp.sum(sq_in[1][...], axis=0, keepdims=True)
            second_sum = jnp.sum(total, axis=0, keepdims=True)
            squares[...] = jnp.where(sub_id() == 0, first_sum, second_sum)
        for target in range(group):
            send[target, 0:4] = jnp.zeros((4, SUB, LANES), F32)
            if not more:
                send[target, 4] = squares[...]
        for slot in range(slots):
            target = table[rank, COLS * slot]

            @pl.when(target < group)
            def _():
                def write(quad, packed):
                    send[target, quad] = packed

                block = [table[rank, COLS * slot + 1 + index] for index in range(3)]
                extract(potential, write, *block)

        if more:
            low = potential[0:WIDE]
            high = potential[ex - WIDE : ex]
            side_a[0] = jnp.where(odd, low, high)
            side_b[0] = jnp.where(odd, high, low)

    return body


def work(
    coarse_source,
    coarse_shift,
    coarse_start,
    fine_source,
    fine_shift,
    fine_start,
    box_corner,
    box_owner,
):
    ex, ey, ez = coarse_source.shape
    size_x, size_y, size_z = (lax.axis_size(axis) for axis in ("gx", "gy", "gz"))
    group = size_y * size_z
    slots, fine = fine_source.shape
    nbx, nby, nbz = ex // FOOT, ey // FOOT, ez // FOOT
    nt = ey // SUB
    assert ez == LANES and nby > 1 and fine == SIDE**3
    both = size_z > 2
    span = ex + 2 * WIDE
    sizes = (size_x, size_y, size_z)
    corner = jnp.transpose(box_corner, (2, 0, 1))

    def tiled(field):
        return field.reshape(ex, nt, SUB, LANES)

    def rows(field):
        count = fine // LANES
        return field.reshape(slots, count, LANES).transpose(1, 0, 2).reshape(count * slots, LANES)

    def exchange(value):
        return lax.all_to_all(value, GROUP_AXES, split_axis=0, concat_axis=0, tiled=True)

    start, shift, source = tiled(coarse_start), tiled(coarse_shift), tiled(coarse_source)
    f_source, f_shift, f_start = rows(fine_source), rows(fine_shift), rows(fine_start)

    def halos(fields, side_a, side_b, outs):
        count = len(fields)
        xa, xb = swap("gx", side_a, side_b)
        place = HBM if count > 1 else VMEM
        ins = [(place, field) for field in fields]
        ya, yb = call(
            y_send_body(count, ex, nt),
            ins + [(VMEM, xa), (VMEM, xb)],
            [(VMEM, out(count, span // 2, SUB, LANES))] * 2,
            [
                pltpu.VMEM((count, 2, ex, SUB, LANES), F32),
                pltpu.SemaphoreType.DMA((count, 2)),
            ],
        )
        ya, yb = swap("gy", ya, yb)
        units = -(-span * (nt + 1) // (LANES // WIDE))
        zs = call(
            z_send_body(count, ex, nt),
            ins + [(VMEM, value) for value in (xa, xb, ya, yb)],
            [(VMEM, out(count, units, SUB, LANES))] * (2 if both else 1),
            [
                pltpu.VMEM((count, ex, nt, SUB, LANES), F32),
                pltpu.SemaphoreType.DMA((count,)),
            ],
        )
        if both:
            zs = list(swap("gz", *zs))
        else:
            zs = [swap("gz", zs[0], zs[0])[0]]
        return call(
            halo_body(count, ex, nt, both, sizes),
            ins + [(VMEM, value) for value in (xa, xb, ya, yb, *zs)],
            [(VMEM, out(span, 2, SUB * (nt + 1), LANES))] * outs,
            [
                pltpu.VMEM((count, ex, nt, SUB, LANES), F32),
                pltpu.SemaphoreType.DMA((count,)),
            ],
        )

    fields = [start, shift, source]
    send, side_a, side_b = call(
        send_start_body((ex, group, slots, nbx, nby, nbz)),
        [(HBM, value) for value in (corner, box_owner, *fields)],
        [(VMEM, out(group, 5, SUB, LANES))] + [(VMEM, out(3, WIDE, nt, SUB, LANES))] * 2,
        [
            pltpu.VMEM((ex, nt, SUB, LANES), F32),
            pltpu.SMEM(corner.shape, jnp.int32),
            pltpu.SMEM(box_owner.shape, jnp.int32),
            pltpu.SemaphoreType.DMA((3,)),
            pltpu.SemaphoreType.DMA((3, 2)),
        ],
    )
    got = exchange(send)
    wide, rate, source_wide = halos(fields, side_a, side_b, 3)

    box_shape = (slots, SIDE, SUB, LANES)
    flat = pltpu.VMEM((slots * fine // LANES, LANES), F32)
    whole = pltpu.VMEM(box_shape, F32)
    ghost = pltpu.VMEM((slots, FOOT, SUB, LANES), F32)
    packs = pltpu.VMEM((slots, 4, SUB, LANES), F32)
    box_scratch = [packs, whole, whole, ghost, whole, whole]
    box_scratch += [pltpu.SMEM((slots, 3), jnp.int32), pltpu.SemaphoreType.DMA((8,))]
    box_outs = [
        (VMEM, out(group, 4 + slots, SUB, LANES)),
        (HBM, out(*box_shape)),
        (VMEM, out(SUB, LANES)),
    ]
    norms = []
    table = None
    for cycle in range(CYCLES):
        first = cycle == 0
        body = fine_body((group, slots, nby, nbz, size_z), first)
        if first:
            ret, state, squares, table, kept, f_rate = call(
                body,
                [(VMEM, got)] + [(HBM, value) for value in (f_source, f_shift, f_start)],
                box_outs
                + [(SMEM, out(group, COLS * slots, dtype=jnp.int32))]
                + [(HBM, out(*box_shape))] * 2,
                box_scratch
                + [
                    pltpu.SMEM((group, LANES), F32),
                    pltpu.SMEM((group + 1,), jnp.int32),
                    pltpu.SemaphoreType.DMA((group,)),
                ]
                + [flat] * 3,
            )
        else:
            ret, state, squares = call(
                body,
                [(SMEM, table), (VMEM, got)]
                + [(HBM, value) for value in (state, kept, f_rate)],
                box_outs,
                box_scratch,
            )
        back = exchange(ret)
        units = (WIDE - 1) * (nt + 1) + 1
        added, side_a, side_b = call(
            place_body((ex, nt, group, slots, size_y, size_z, nby, nbz)),
            [(SMEM, table), (VMEM, back)],
            [(VMEM, out(ex, 2, nt + 1, SUB, LANES))] + [(VMEM, out(units, SUB, LANES))] * 2,
        )
        xa, xb = swap("gx", side_a, side_b)
        more = cycle < CYCLES - 1
        wide_shape = (span, 2, SUB * (nt + 1), LANES)
        result = call(
            coarse_body((ex, nt, group, slots, size_z), more),
            [(SMEM, table)]
            + [(VMEM, v) for v in (wide, rate, source_wide, added, xa, xb, squares, *norms)],
            [
                (VMEM, out(ex, nt, SUB, LANES)),
                (VMEM, out(group, 4 if more else 5, SUB, LANES)),
                (VMEM, out(SUB, LANES)),
            ]
            + [(VMEM, out(1, WIDE, nt, SUB, LANES))] * (2 if more else 0),
            [pltpu.VMEM(wide_shape, F32)] * 3,
        )
        potential, send = result[:2]
        norms.append(result[2])
        got = exchange(send)
        if more:
            (wide,) = halos([potential], result[3], result[4], 1)
    (total,) = call(norm_body(group), [(VMEM, got)], [(VMEM, out(SUB, LANES))])
    (values,) = call(
        last_body((group, slots, size_z)),
        [(SMEM, table), (VMEM, got), (HBM, state)],
        [(HBM, out(slots * fine // LANES, LANES))],
        [packs, ghost, whole, flat, pltpu.SemaphoreType.DMA((2,))],
    )
    cells = float(ex * ey * ez * size_x * size_y * size_z)
    bit = 1
    while bit < size_x:
        pairs = [(i, i ^ bit) for i in range(size_x)]
        total = total + lax.ppermute(total, "gx", pairs)
        bit *= 2
    total = jnp.sum(total[:CYCLES], axis=1)
    values = values.reshape(fine // LANES, slots, LANES).transpose(1, 0, 2).reshape(slots, fine)
    return potential.reshape(ex, ey, ez), values, jnp.sqrt(total / cells)


def solution(mesh):
    in_specs = (
        P("gx", "gy", "gz"),
        P("gx", "gy", "gz"),
        P("gx", "gy", "gz"),
        P(("gx", "gy", "gz"), None),
        P(("gx", "gy", "gz"), None),
        P(("gx", "gy", "gz"), None),
        P(("gx", "gy", "gz"), None, None),
        P(("gx", "gy", "gz"), None),
    )
    out_specs = (P("gx", "gy", "gz"), P(("gx", "gy", "gz"), None), P())
    return jax.shard_map(work, mesh=mesh, in_specs=in_specs, out_specs=out_specs, check_vma=False)
```

```python
import jax
import jax.numpy as jnp
from jax import lax
from jax.experimental import pallas as pl
from jax.experimental.pallas import tpu as pltpu
from jax.sharding import PartitionSpec as P


FOOT = 16
CYCLES = 2
CSWEEPS = 4
FSWEEPS = 3
OMEGA = 0.8

SUB = 8
LANES = 128
SIDE = 2 * FOOT
WIDE = 4
COLS = 8
GROUP_AXES = ("gy", "gz")

VMEM = pl.BlockSpec(memory_space=pltpu.VMEM)
SMEM = pl.BlockSpec(memory_space=pltpu.SMEM)
HBM = pl.BlockSpec(memory_space=pltpu.HBM)
F32 = jnp.float32


def out(*shape, dtype=F32):
    return jax.ShapeDtypeStruct(shape, dtype)


def call(body, ins, outs, scratch=()):
    values = [
        pltpu.with_memory_space_constraint(value, pltpu.HBM) if spec is HBM else value
        for spec, value in ins
    ]
    shapes = [pltpu.HBM(shape.shape, shape.dtype) if spec is HBM else shape for spec, shape in outs]
    return pl.pallas_call(
        body,
        in_specs=[spec for spec, _ in ins],
        out_specs=[spec for spec, _ in outs],
        out_shape=shapes,
        scratch_shapes=list(scratch),
        compiler_params=pltpu.CompilerParams(vmem_limit_bytes=16 << 20),
    )(*values)


def place_of():
    return [lax.axis_index(axis) for axis in ("gx", "gy", "gz")]


def fetch(copies):
    for copy in copies:
        copy.start()
    return copies


def arrive(copies):
    for copy in copies:
        copy.wait()


def lane_id():
    return lax.broadcasted_iota(jnp.int32, (SUB, LANES), 1)


def sub_id():
    return lax.broadcasted_iota(jnp.int32, (SUB, LANES), 0)


def gather(values, index, axis):
    return jnp.take_along_axis(values, index, axis=axis)


def swap_pairs(count):
    first = [(i, i ^ 1) for i in range(count)]
    second = [(i, (i + 1) % count if i % 2 else (i - 1) % count) for i in range(count)]
    return first, second


def swap(axis, first, second):
    count = lax.axis_size(axis)
    pairs_a, pairs_b = swap_pairs(count)
    got_a = lax.ppermute(first, axis, pairs_a)
    got_b = lax.ppermute(second, axis, pairs_b) if count > 2 else got_a
    return got_a, got_b


def pick_low(odd, got_a, got_b):
    return jnp.where(odd, got_a, got_b)


def pick_high(odd, got_a, got_b):
    return jnp.where(odd, got_b, got_a)


def extract(field, write, block_x, block_y, block_z):
    lanes = lane_id() // FOOT
    for quad in range(FOOT // 4):
        packed = None
        for inner in range(4):
            for part in range(FOOT // SUB):
                piece = field[FOOT * block_x + 4 * quad + inner, block_y * (FOOT // SUB) + part]
                spot = 2 * inner + part
                piece = pltpu.roll(piece, (FOOT * spot + LANES - FOOT * block_z) % LANES, 1)
                packed = piece if packed is None else jnp.where(lanes == spot, piece, packed)
        write(quad, packed)


def send_start_body(dims):
    ex, group, slots, nbx, nby, nbz = dims

    def body(
        corner_in, owner_in, field, shift, source, send, side_a, side_b, start, corner, owner, sem, sems
    ):
        small = [
            pltpu.make_async_copy(corner_in, corner, sem.at[1]),
            pltpu.make_async_copy(owner_in, owner, sem.at[2]),
        ]
        fetch(small)
        copy = pltpu.make_async_copy(field, start, sem.at[0])
        copy.start()
        odd = lax.axis_index("gx") % 2
        sides = []
        for index, raw in enumerate((field, shift, source)):
            for side, goal in enumerate((side_a, side_b)):
                high = 1 - odd if side == 0 else odd
                planes = raw.at[pl.ds(high * (ex - WIDE), WIDE)]
                sides.append(pltpu.make_async_copy(planes, goal.at[index], sems.at[index, side]))
        fetch(sides)
        arrive(small)
        pos = place_of()
        lanes = lane_id()
        note = jnp.zeros((SUB, LANES), F32)
        blocks = []
        for slot in range(slots):
            block = (
                corner[0, 0, slot] // SIDE - pos[0] * nbx,
                corner[1, 0, slot] // SIDE - pos[1] * nby,
                corner[2, 0, slot] // SIDE - pos[2] * nbz,
            )
            blocks.append(block)
            for index, value in enumerate((owner[0, slot],) + block):
                note = jnp.where(lanes == 4 * slot + index, value.astype(F32), note)
        for target in range(group):
            send[target, 0:4] = jnp.zeros((4, SUB, LANES), F32)
            send[target, 4] = note
        copy.wait()
        for slot in range(slots):
            target = owner[0, slot]

            @pl.when(target < group)
            def _():
                def write(quad, packed):
                    send[target, quad] = packed

                extract(start, write, *blocks[slot])

        arrive(sides)

    return body


def x_plane(field, got_a, got_b, odd, ex, xi):
    if xi < WIDE:
        return pick_low(odd, got_a[xi], got_b[xi])
    if xi < ex + WIDE:
        return field[xi - WIDE]
    return pick_high(odd, got_a[xi - ex - WIDE], got_b[xi - ex - WIDE])


def y_send_body(count, ex, nt):
    def body(*refs):
        fields, (xa, xb, ya, yb) = refs[:count], refs[count : count + 4]
        planes, sems = refs[count + 4 :]
        pos = place_of()
        odd_x = pos[0] % 2 == 1
        odd_y = pos[1] % 2 == 1
        copies = []
        for index in range(count):
            for side in range(2):
                tile = fields[index].at[:, side * (nt - 1)]
                copies.append(
                    pltpu.make_async_copy(tile, planes.at[index, side], sems.at[index, side])
                )
        fetch(copies)
        rows = sub_id()

        def pair(index, xi):
            found = []
            for at in (xi, xi + 1):
                if WIDE <= at < WIDE + ex:
                    found.append((planes[index, 0, at - WIDE], planes[index, 1, at - WIDE]))
                else:
                    plane = x_plane(None, xa.at[index], xb.at[index], odd_x, ex, at)
                    found.append((plane[0], plane[nt - 1]))
            (low, high), (low_next, high_next) = found
            low = jnp.where(rows < WIDE, low, pltpu.roll(low_next, WIDE, 0))
            high = jnp.where(rows < WIDE, pltpu.roll(high, WIDE, 0), high_next)
            ya[index, xi // 2] = jnp.where(odd_y, low, high)
            yb[index, xi // 2] = jnp.where(odd_y, high, low)

        edges = [*range(0, WIDE, 2), *range(WIDE + ex, 2 * WIDE + ex, 2)]
        for index in range(count):
            for xi in edges:
                pair(index, xi)
        arrive(copies)
        for index in range(count):
            for xi in range(WIDE, WIDE + ex, 2):
                pair(index, xi)

    return body


def seam_tile(ya, yb, odd_y, xi):
    low = pick_low(odd_y, ya[xi // 2], yb[xi // 2])
    high = pick_high(odd_y, ya[xi // 2], yb[xi // 2])
    if xi % 2 == 0:
        low = pltpu.roll(low, WIDE, 0)
    else:
        high = pltpu.roll(high, WIDE, 0)
    return jnp.where(sub_id() < WIDE, high, low)


def z_send_body(count, ex, nt):
    def body(*refs):
        raw, (xa, xb, ya, yb) = refs[:count], refs[count : count + 4]
        outs = refs[count + 4 : -2]
        fields, sems = refs[-2:]
        copies = [
            pltpu.make_async_copy(raw[index], fields.at[index], sems.at[index])
            for index in range(count)
        ]
        arrive(fetch(copies))
        pos = place_of()
        odd_x = pos[0] % 2 == 1
        odd_y = pos[1] % 2 == 1
        odd_z = pos[2] % 2
        lanes = lane_id() // WIDE
        per = LANES // WIDE
        for index in range(count):
            unit = 0
            packed = [None] * len(outs)
            total = (ex + 2 * WIDE) * (nt + 1)
            for xi in range(ex + 2 * WIDE):
                plane = x_plane(fields.at[index], xa.at[index], xb.at[index], odd_x, ex, xi)
                for tile in range(nt + 1):
                    if tile < nt:
                        value = plane[tile]
                    else:
                        value = seam_tile(ya.at[index], yb.at[index], odd_y, xi)
                    spot = unit % per
                    for which in range(len(outs)):
                        high = 1 - odd_z if which == 0 else odd_z
                        moved = pltpu.roll(value, (WIDE * spot + WIDE * high) % LANES, 1)
                        if spot == 0:
                            packed[which] = moved
                        else:
                            packed[which] = jnp.where(lanes == spot, moved, packed[which])
                        if spot == per - 1 or unit == total - 1:
                            outs[which][index, unit // per] = packed[which]
                    unit += 1

    return body


def halo_body(count, ex, nt, both, sizes):
    ny_rows = SUB * nt

    def inside_xy(pos, xi, tile):
        gx = pos[0] * ex + xi - WIDE
        ok = (gx >= 0) & (gx < sizes[0] * ex)
        row = sub_id()
        if tile < nt:
            return ok, None
        y = pos[1] * ny_rows + jnp.where(row < WIDE, ny_rows + row, row - SUB)
        return ok, (y >= 0) & (y < sizes[1] * ny_rows)

    def body(*refs):
        raw, (xa, xb, ya, yb) = refs[:count], refs[count : count + 4]
        rest = refs[count + 4 : -2]
        zs, outs = (rest[:2], rest[2:]) if both else (rest[:1], rest[1:])
        fields, sems = refs[-2:]
        copies = [
            pltpu.make_async_copy(raw[index], fields.at[index], sems.at[index])
            for index in range(count)
        ]
        arrive(fetch(copies))
        pos = place_of()
        odd_x = pos[0] % 2 == 1
        odd_y = pos[1] % 2 == 1
        odd_z = pos[2] % 2
        lanes = lane_id()
        per = LANES // WIDE
        has_high = pos[2] < sizes[2] - 1
        has_low = pos[2] > 0
        z_mask = ((lanes < WIDE) & has_high) | ((lanes >= LANES - WIDE) & has_low)
        unit = 0
        for xi in range(ex + 2 * WIDE):
            planes = [
                x_plane(fields.at[index], xa.at[index], xb.at[index], odd_x, ex, xi)
                for index in range(count)
            ]
            for tile in range(nt + 1):
                ok, rows = inside_xy(pos, xi, tile)
                if rows is None:
                    good = jnp.broadcast_to(ok, (SUB, LANES))
                else:
                    good = rows & ok
                spot = unit % per
                for index in range(count):
                    if tile < nt:
                        main = planes[index][tile]
                    else:
                        main = seam_tile(ya.at[index], yb.at[index], odd_y, xi)
                    parts = []
                    for which in range(len(zs)):
                        high = 1 - odd_z if which == 0 else odd_z
                        shift = (LANES - WIDE * spot + LANES - WIDE * (1 - high)) % LANES
                        parts.append(pltpu.roll(zs[which][index, unit // per], shift, 1))
                    if len(parts) == 1:
                        halo = parts[0]
                    else:
                        halo = jnp.where(
                            lanes < LANES // 2,
                            jnp.where(odd_z == 1, parts[1], parts[0]),
                            jnp.where(odd_z == 1, parts[0], parts[1]),
                        )
                    where_main = (xi, 0, slice(SUB * tile, SUB * tile + SUB))
                    where_halo = (xi, 1, slice(SUB * tile, SUB * tile + SUB))
                    if index == 0:
                        outs[0][where_main] = jnp.where(good, main, 0.0)
                        outs[0][where_halo] = jnp.where(good & z_mask, halo, 0.0)
                    elif index == 1:
                        outs[1][where_main] = jnp.where(good, OMEGA / (6.0 + main), 0.0)
                        diag = 6.0 + jnp.where(z_mask, halo, 0.0)
                        outs[1][where_halo] = jnp.where(good & z_mask, OMEGA / diag, 0.0)
                    else:
                        outs[2][where_main] = main
                        outs[2][where_halo] = jnp.where(z_mask, halo, 0.0)
                unit += 1

    return body


def around(value, ghost, masks):
    below, above, low_lanes, high_lanes, first, last = masks
    total = jnp.where(below, ghost, pltpu.roll(value, 1, 1))
    total = total + jnp.where(above, ghost, pltpu.roll(value, LANES - 1, 1))
    moved = pltpu.roll(value, SIDE, 1)
    moved = jnp.where(low_lanes, pltpu.roll(moved, 1, 0), moved)
    total = total + jnp.where(first, ghost, moved)
    moved = pltpu.roll(value, LANES - SIDE, 1)
    moved = jnp.where(high_lanes, pltpu.roll(moved, SUB - 1, 0), moved)
    return total + jnp.where(last, ghost, moved)


def fine_masks():
    lanes, rows = lane_id(), sub_id()
    low_lanes = lanes < SIDE
    high_lanes = lanes >= LANES - SIDE
    return (
        lanes % SIDE == 0,
        lanes % SIDE == SIDE - 1,
        low_lanes,
        high_lanes,
        low_lanes & (rows == 0),
        high_lanes & (rows == SUB - 1),
    )


def assign(rank, table, group, slots, found):
    count = jnp.int32(0)
    for home in range(group):
        for slot in range(slots):
            hit = table[home, COLS * slot] == rank

            @pl.when(hit)
            def _():
                found(count, home, slot)

            count = count + hit.astype(jnp.int32)
    return count


def unpack(packed, ghosts, slots):
    lanes, rows = lane_id(), sub_id()
    column = (lanes % SIDE) // 2
    row = (2 * rows + lanes // (LANES // 2)) % SUB
    upper = rows >= SUB // 2

    def box(index, carry):
        for quad in range(FOOT // 4):
            value = packed[index, quad]
            for inner in range(4):
                low = gather(value, 32 * inner + column, 1)
                high = gather(value, 32 * inner + FOOT + column, 1)
                plane = jnp.where(upper, gather(high, row, 0), gather(low, row, 0))
                ghosts[index, 4 * quad + inner] = plane
        return carry

    lax.fori_loop(0, slots, box, 0)


def fine_body(dims, first):
    group, slots, _, _, size_z = dims

    def body(*refs):
        if first:
            got, *stored = refs[:4]
            ret, state_out, squares, table_out, kept_out, rate_out = refs[4:10]
            packed, other, state, ghosts, kept, rate, homes, table, moved = refs[10:19]
            copied, counts, sems = refs[19:22]
            old = refs[22:]
        else:
            table_in, got, *stored = refs[:5]
            ret, state_out, squares = refs[5:8]
            packed, other, state, ghosts, kept, rate, homes, table, moved = refs[8:]
            tables = [pltpu.make_async_copy(table_in, table, moved.at[5])]
            fetch(tables)
            old = (other, kept, rate)
        loads = [
            pltpu.make_async_copy(source, goal, moved.at[index])
            for index, (source, goal) in enumerate(zip(stored, old))
        ]
        rank = lax.axis_index("gy") * size_z + lax.axis_index("gz")
        if first:
            for home in range(group):
                pltpu.make_async_copy(got.at[home, 4, 0], copied.at[home], sems.at[home]).start()
        fetch(loads)
        packed[...] = jnp.zeros(packed.shape, F32)
        if first:
            for home in range(group):
                pltpu.make_async_copy(got.at[home, 4, 0], copied.at[home], sems.at[home]).wait()
            for owner in range(group):
                counts[owner] = jnp.int32(0)
            for home in range(group):
                for slot in range(slots):
                    for index in range(4):
                        value = copied[home, 4 * slot + index].astype(jnp.int32)
                        table[home, COLS * slot + index] = value
                    owner = jnp.minimum(table[home, COLS * slot], group)
                    place = counts[owner]
                    table[home, COLS * slot + 4] = place
                    counts[owner] = place + 1

        if not first:
            arrive(tables)

        def found(count, home, slot):
            packed[count] = got[home, 0:4]
            homes[count, 0] = jnp.int32(home)
            homes[count, 1] = table[home, COLS * slot + 2]
            homes[count, 2] = table[home, COLS * slot + 3]

        for slot in range(slots):
            homes[slot, 0] = jnp.int32(0)
            homes[slot, 1] = jnp.int32(0)
            homes[slot, 2] = jnp.int32(0)
        live = assign(rank, table, group, slots, found)
        unpack(packed, ghosts, slots)
        saves = []
        arrive(loads if first else loads[:1])
        masks = fine_masks()
        lanes, rows = lane_id(), sub_id()

        def convert(index, carry):
            for x in range(SIDE):
                at = pl.ds(SIDE * x + index, SUB, stride=slots)
                kept[index, x] = old[0][at, :]
                rate[index, x] = OMEGA / (6.0 + old[1][at, :])
                other[index, x] = old[2][at, :]
            return carry

        if first:
            lax.fori_loop(0, slots, convert, 0)
            saves.append(pltpu.make_async_copy(table, table_out, moved.at[5]))
            saves.append(pltpu.make_async_copy(kept, kept_out, moved.at[6]))
            saves.append(pltpu.make_async_copy(rate, rate_out, moved.at[7]))
            fetch(saves)

        def begin(index, carry):
            for x in range(SIDE):
                other[index, x] = other[index, x] + ghosts[index, x // 2]
            return carry

        if not first:
            lax.fori_loop(0, slots, begin, 0)
            arrive(loads[1:])

        def residual(buffer, index, x):
            value = buffer[index, x]
            ghost = ghosts[index, x // 2]
            near = around(value, ghost, masks)
            near = near + (buffer[index, x - 1] if x > 0 else ghost)
            near = near + (buffer[index, x + 1] if x < SIDE - 1 else ghost)
            return value, kept[index, x] + near

        buffers = [other, state, other, state]
        for sweep in range(FSWEEPS):
            here, there = buffers[sweep], buffers[sweep + 1]

            def step(index, carry):
                for x in range(SIDE):
                    value, rest = residual(here, index, x)
                    there[index, x] = (1.0 - OMEGA) * value + rate[index, x] * rest
                return carry

            lax.fori_loop(0, slots, step, 0)
        final = state

        def save(index):
            return pltpu.make_async_copy(other.at[index], state_out.at[index], moved.at[index])

        def remainder(index, x):
            value, rest = residual(final, index, x)
            other[index, x] = value - ghosts[index, x // 2]
            return rest - (OMEGA / rate[index, x]) * value


        def finish(index, total):
            zone_y = jnp.where(homes[index, 1] == 0, 0, SUB - 2)
            zone_z = jnp.where(homes[index, 2] == 0, 0, FOOT - WIDE)
            column = (rows % 2) * (LANES // 2)
            take_all = column + 2 * (lanes % FOOT)
            take_z = column + 2 * (zone_z + lanes % WIDE)
            row_y = zone_y + (rows % 4) // 2
            row_low = rows // 2
            row_high = SUB // 2 + rows // 2
            mine = jnp.zeros((SUB, LANES), F32)
            y_slab = jnp.zeros((SUB, LANES), F32)
            z_slab = jnp.zeros((SUB, LANES), F32)
            whole = None
            for xp in range(FOOT):
                left = remainder(index, 2 * xp)
                mine = mine + left * left
                right = remainder(index, 2 * xp + 1)
                mine = mine + right * right
                both = left + right
                both = both + pltpu.roll(both, LANES - 1, 1)
                both = 0.125 * (both + pltpu.roll(both, LANES - SIDE, 1))
                piece = gather(gather(both, row_y, 0), take_all, 1)
                y_slab = jnp.where((lanes // FOOT == xp // 2) & (rows // 4 == xp % 2), piece, y_slab)
                for part in range(2):
                    picked = gather(both, row_high if part else row_low, 0)
                    piece = gather(picked, take_all, 1)
                    spot = 2 * (xp % 4) + part
                    whole = piece if spot == 0 else jnp.where(lanes // FOOT == spot, piece, whole)
                    piece = gather(picked, take_z, 1)
                    z_slab = jnp.where(lanes // WIDE == 2 * xp + part, piece, z_slab)
                if xp % 4 == 3:
                    packed[index, xp // 4] = whole
            save(index).start()
            home_z = homes[index, 0] % size_z
            for target in range(group):
                ret[target, 4 + index] = jnp.where(home_z == target % size_z, y_slab, z_slab)
            return total + jnp.where(index < live, mine, 0.0)

        squares[...] = lax.fori_loop(0, slots, finish, jnp.zeros((SUB, LANES), F32))
        for target in range(group):
            ret[target, 0:4] = jnp.zeros((4, SUB, LANES), F32)
        for index in range(slots):

            @pl.when(index < live)
            def _():
                ret[homes[index, 0], 0:4] = packed[index]

        arrive(saves)
        arrive([save(index) for index in range(slots)])

    return body


def last_body(dims):
    group, slots, size_z = dims

    def body(table_in, got, old_state, goal, packed, fresh, state, result, table, sems):
        tables = fetch([pltpu.make_async_copy(table_in, table, sems.at[2])])
        loads = [pltpu.make_async_copy(old_state, state, sems.at[0])]
        fetch(loads)
        rank = lax.axis_index("gy") * size_z + lax.axis_index("gz")
        packed[...] = jnp.zeros(packed.shape, F32)

        def found(count, home, slot):
            packed[count] = got[home, 0:4]

        arrive(tables)
        live = assign(rank, table, group, slots, found)
        unpack(packed, fresh, slots)
        arrive(loads)

        def box(index, carry):
            for x in range(SIDE):
                value = state[index, x] + fresh[index, x // 2]
                value = jnp.where(index < live, value, 0.0)
                result[pl.ds(SIDE * x + index, SUB, stride=slots), :] = value
            return carry

        lax.fori_loop(0, slots, box, 0)
        arrive(fetch([pltpu.make_async_copy(result, goal, sems.at[1])]))

    return body


def norm_body(group):
    def body(got, total):
        result = got[0, 4]
        for peer in range(1, group):
            result = result + got[peer, 4]
        total[...] = result

    return body


def place_body(dims):
    ex, nt, group, slots, size_y, size_z, nby, nbz = dims
    tiles = FOOT // SUB

    def body(table_in, got, added, side_a, side_b, table, sem):
        tables = fetch([pltpu.make_async_copy(table_in, table, sem)])
        pos = place_of()
        odd = pos[0] % 2 == 1
        rank = pos[1] * size_z + pos[2]
        lanes, rows = lane_id(), sub_id()
        added[...] = jnp.zeros(added.shape, F32)
        arrive(tables)

        def own(slot, carry):
            owner = table[rank, COLS * slot]

            @pl.when(owner < group)
            def _():
                base_x = FOOT * table[rank, COLS * slot + 1]
                base_y = tiles * table[rank, COLS * slot + 2]
                base_z = FOOT * table[rank, COLS * slot + 3]
                keep = (lanes >= base_z) & (lanes < base_z + FOOT)
                for quad in range(4):
                    value = got[owner, quad]
                    for inner in range(4):
                        for part in range(tiles):
                            spot = 2 * inner + part
                            moved = pltpu.roll(value, (base_z + LANES - FOOT * spot) % LANES, 1)
                            at = (base_x + 4 * quad + inner, 0, base_y + part)
                            added[at] = added[at] + jnp.where(keep, moved, 0.0)

            return carry

        lax.fori_loop(0, slots, own, 0)

        for dy in (-1, 0, 1):
            for dz in (-1, 0, 1):
                if dy == 0 and dz == 0:
                    continue
                home_y = pos[1] + dy
                home_z = pos[2] + dz
                exists = (home_y >= 0) & (home_y < size_y) & (home_z >= 0) & (home_z < size_z)
                home = jnp.where(exists, home_y * size_z + home_z, 0)

                def near(slot, carry):
                    owner = table[home, COLS * slot]
                    block_y = table[home, COLS * slot + 2]
                    block_z = table[home, COLS * slot + 3]
                    wanted = exists & (owner < group)
                    if dy != 0:
                        wanted = wanted & (block_y == (nby - 1 if dy < 0 else 0))
                    if dz != 0:
                        wanted = wanted & (block_z == (nbz - 1 if dz < 0 else 0))

                    @pl.when(wanted)
                    def _():
                        value = got[owner, 4 + table[home, COLS * slot + 4]]
                        base_x = FOOT * table[home, COLS * slot + 1]
                        goal = 0 if dy > 0 else 1
                        if dz == 0:
                            base_z = FOOT * block_z
                            keep = (lanes >= base_z) & (lanes < base_z + FOOT)
                            keep = keep & (rows // 4 == goal)
                            turned = pltpu.roll(value, 4, 0)
                            for x in range(FOOT):
                                use = value if x % 2 == goal else turned
                                shift = (base_z + LANES - FOOT * (x // 2)) % LANES
                                moved = pltpu.roll(use, shift, 1)
                                at = (base_x + x, 0, nt)
                                added[at] = added[at] + jnp.where(keep, moved, 0.0)
                        else:
                            where_z = 0 if dz > 0 else LANES - WIDE
                            keep = (lanes >= where_z) & (lanes < where_z + WIDE)
                            for x in range(FOOT):
                                for part in range(tiles):
                                    shift = (where_z + LANES - WIDE * (2 * x + part)) % LANES
                                    if dy == 0:
                                        moved = pltpu.roll(value, shift, 1)
                                        at = (base_x + x, 1, tiles * block_y + part)
                                        added[at] = added[at] + jnp.where(keep, moved, 0.0)
                                    elif part == (0 if dy > 0 else tiles - 1):
                                        moved = pltpu.roll(value, shift, 1)
                                        both = keep & (rows // 4 == goal)
                                        at = (base_x + x, 1, nt)
                                        added[at] = added[at] + jnp.where(both, moved, 0.0)

                    return carry

                lax.fori_loop(0, slots, near, 0)

        for low_side in (True, False):
            packed = None
            for index in range(WIDE - 1):
                plane = index if low_side else ex - (WIDE - 1) + index
                for tile in range(nt + 1):
                    spot = index * (nt + 1) + tile
                    moved = pltpu.roll(added[plane, 1, tile], WIDE + 2 * WIDE * spot, 1)
                    if spot == 0:
                        packed = moved
                    else:
                        packed = jnp.where(lanes // (2 * WIDE) == spot, moved, packed)
            units = (WIDE - 1) * (nt + 1)
            if low_side:
                low_packed = packed
            else:
                high_packed = packed
        for index in range(WIDE - 1):
            for tile in range(nt + 1):
                low = added[index, 0, tile]
                high = added[ex - (WIDE - 1) + index, 0, tile]
                spot = index * (nt + 1) + tile
                side_a[spot] = jnp.where(odd, low, high)
                side_b[spot] = jnp.where(odd, high, low)
        side_a[units] = jnp.where(odd, low_packed, high_packed)
        side_b[units] = jnp.where(odd, high_packed, low_packed)

    return body


def coarse_body(dims, more):
    ex, nt, group, slots, size_z = dims
    span = ex + 2 * WIDE
    rows_all = SUB * (nt + 1)

    def body(table_in, wide, rate, source, added, xa, xb, *refs):
        pos = place_of()
        sq_in, refs = refs[: 1 if more else 2], refs[1 if more else 2 :]
        if more:
            potential, send, squares, side_a, side_b = refs[:5]
        else:
            potential, send, squares = refs[:3]
        comp, one, two, table, sem = refs[-5:]
        tables = fetch([pltpu.make_async_copy(table_in, table, sem)])
        odd = pos[0] % 2 == 1
        rank = pos[1] * size_z + pos[2]
        lanes = lane_id()
        halo_lanes = (lanes < WIDE) | (lanes >= LANES - WIDE)
        units = (WIDE - 1) * (nt + 1)

        def fill(x, carry):
            for zone in range(2):
                for tile in range(nt + 1):
                    at = (WIDE + x, zone, pl.ds(SUB * tile, SUB))
                    comp[at] = source[at] + added[x, zone, tile]
            return carry

        lax.fori_loop(0, ex, fill, 0, unroll=True)
        low_tail = pick_low(odd, xa[units], xb[units])
        high_tail = pick_high(odd, xa[units], xb[units])
        for index in range(WIDE - 1):
            for tile in range(nt + 1):
                spot = index * (nt + 1) + tile
                shift = (LANES - WIDE - 2 * WIDE * spot) % LANES
                rows = slice(SUB * tile, SUB * tile + SUB)
                xi = 1 + index
                comp[xi, 0, rows] = source[xi, 0, rows] + pick_low(odd, xa[spot], xb[spot])
                tail = jnp.where(halo_lanes, pltpu.roll(low_tail, shift, 1), 0.0)
                comp[xi, 1, rows] = source[xi, 1, rows] + tail
                xi = WIDE + ex + index
                comp[xi, 0, rows] = source[xi, 0, rows] + pick_high(odd, xa[spot], xb[spot])
                tail = jnp.where(halo_lanes, pltpu.roll(high_tail, shift, 1), 0.0)
                comp[xi, 1, rows] = source[xi, 1, rows] + tail

        edge = lax.broadcasted_iota(jnp.int32, (rows_all, LANES), 1)

        def update(here, xi):
            main, halo = here[xi, 0], here[xi, 1]
            main_up, halo_up = pltpu.roll(main, 1, 1), pltpu.roll(halo, 1, 1)
            main_dn, halo_dn = pltpu.roll(main, LANES - 1, 1), pltpu.roll(halo, LANES - 1, 1)
            at_low, at_high = edge == 0, edge == LANES - 1
            result = []
            for zone, value in ((0, main), (1, halo)):
                if zone == 0:
                    near = jnp.where(at_low, halo_up, main_up) + jnp.where(at_high, halo_dn, main_dn)
                else:
                    near = jnp.where(at_low, main_up, halo_up) + jnp.where(at_high, main_dn, halo_dn)
                near = near + pltpu.roll(value, 1, 0) + pltpu.roll(value, rows_all - 1, 0)
                near = near + here[xi - 1, zone] + here[xi + 1, zone]
                rest = comp[xi, zone] + near
                result.append((value, rest))
            return result

        buffers = [wide, one, two, one]
        for sweep in range(CSWEEPS - 1):
            here, there = buffers[sweep], buffers[sweep + 1]

            def step(xi, carry):
                for zone, (value, rest) in enumerate(update(here, xi)):
                    there[xi, zone] = (1.0 - OMEGA) * value + rate[xi, zone] * rest
                return carry

            lax.fori_loop(1 + sweep, span - 1 - sweep, step, 0, unroll=True)
        here = buffers[CSWEEPS - 1]

        def step(x, total):
            value, rest = update(here, WIDE + x)[0]
            weight = rate[WIDE + x, 0]
            rest = rest - (OMEGA / weight) * value
            value = value + weight * rest
            for tile in range(nt):
                rows = slice(SUB * tile, SUB * tile + SUB)
                potential[x, tile] = value[rows]
                total = total + rest[rows] * rest[rows]
            return total

        total = lax.fori_loop(0, ex, step, sq_in[0][...], unroll=True)
        if more:
            squares[...] = total
        else:
            first_sum = jnp.sum(sq_in[1][...], axis=0, keepdims=True)
            second_sum = jnp.sum(total, axis=0, keepdims=True)
            squares[...] = jnp.where(sub_id() == 0, first_sum, second_sum)
        for target in range(group):
            send[target, 0:4] = jnp.zeros((4, SUB, LANES), F32)
            if not more:
                send[target, 4] = squares[...]
        arrive(tables)
        for slot in range(slots):
            target = table[rank, COLS * slot]

            @pl.when(target < group)
            def _():
                def write(quad, packed):
                    send[target, quad] = packed

                block = [table[rank, COLS * slot + 1 + index] for index in range(3)]
                extract(potential, write, *block)

        if more:
            low = potential[0:WIDE]
            high = potential[ex - WIDE : ex]
            side_a[0] = jnp.where(odd, low, high)
            side_b[0] = jnp.where(odd, high, low)

    return body


def work(
    coarse_source,
    coarse_shift,
    coarse_start,
    fine_source,
    fine_shift,
    fine_start,
    box_corner,
    box_owner,
):
    ex, ey, ez = coarse_source.shape
    size_x, size_y, size_z = (lax.axis_size(axis) for axis in ("gx", "gy", "gz"))
    group = size_y * size_z
    slots, fine = fine_source.shape
    nbx, nby, nbz = ex // FOOT, ey // FOOT, ez // FOOT
    nt = ey // SUB
    assert ez == LANES and nby > 1 and fine == SIDE**3
    both = size_z > 2
    span = ex + 2 * WIDE
    sizes = (size_x, size_y, size_z)
    corner = jnp.transpose(box_corner, (2, 0, 1))

    def tiled(field):
        return field.reshape(ex, nt, SUB, LANES)

    def rows(field):
        count = fine // LANES
        return field.reshape(slots, count, LANES).transpose(1, 0, 2).reshape(count * slots, LANES)

    def exchange(value):
        return lax.all_to_all(value, GROUP_AXES, split_axis=0, concat_axis=0, tiled=True)

    start, shift, source = tiled(coarse_start), tiled(coarse_shift), tiled(coarse_source)
    f_source, f_shift, f_start = rows(fine_source), rows(fine_shift), rows(fine_start)

    def halos(fields, side_a, side_b, outs):
        count = len(fields)
        xa, xb = swap("gx", side_a, side_b)
        place = HBM if count > 1 else VMEM
        ins = [(place, field) for field in fields]
        ya, yb = call(
            y_send_body(count, ex, nt),
            ins + [(VMEM, xa), (VMEM, xb)],
            [(VMEM, out(count, span // 2, SUB, LANES))] * 2,
            [
                pltpu.VMEM((count, 2, ex, SUB, LANES), F32),
                pltpu.SemaphoreType.DMA((count, 2)),
            ],
        )
        ya, yb = swap("gy", ya, yb)
        units = -(-span * (nt + 1) // (LANES // WIDE))
        zs = call(
            z_send_body(count, ex, nt),
            ins + [(VMEM, value) for value in (xa, xb, ya, yb)],
            [(VMEM, out(count, units, SUB, LANES))] * (2 if both else 1),
            [
                pltpu.VMEM((count, ex, nt, SUB, LANES), F32),
                pltpu.SemaphoreType.DMA((count,)),
            ],
        )
        if both:
            zs = list(swap("gz", *zs))
        else:
            zs = [swap("gz", zs[0], zs[0])[0]]
        return call(
            halo_body(count, ex, nt, both, sizes),
            ins + [(VMEM, value) for value in (xa, xb, ya, yb, *zs)],
            [(VMEM, out(span, 2, SUB * (nt + 1), LANES))] * outs,
            [
                pltpu.VMEM((count, ex, nt, SUB, LANES), F32),
                pltpu.SemaphoreType.DMA((count,)),
            ],
        )

    fields = [start, shift, source]
    send, side_a, side_b = call(
        send_start_body((ex, group, slots, nbx, nby, nbz)),
        [(HBM, value) for value in (corner, box_owner, *fields)],
        [(VMEM, out(group, 5, SUB, LANES))] + [(VMEM, out(3, WIDE, nt, SUB, LANES))] * 2,
        [
            pltpu.VMEM((ex, nt, SUB, LANES), F32),
            pltpu.SMEM(corner.shape, jnp.int32),
            pltpu.SMEM(box_owner.shape, jnp.int32),
            pltpu.SemaphoreType.DMA((3,)),
            pltpu.SemaphoreType.DMA((3, 2)),
        ],
    )
    got = exchange(send)
    wide, rate, source_wide = halos(fields, side_a, side_b, 3)

    box_shape = (slots, SIDE, SUB, LANES)
    flat = pltpu.VMEM((slots * fine // LANES, LANES), F32)
    whole = pltpu.VMEM(box_shape, F32)
    ghost = pltpu.VMEM((slots, FOOT, SUB, LANES), F32)
    packs = pltpu.VMEM((slots, 4, SUB, LANES), F32)
    box_scratch = [packs, whole, whole, ghost, whole, whole]
    routes = pltpu.SMEM((group, COLS * slots), jnp.int32)
    box_scratch += [pltpu.SMEM((slots, 3), jnp.int32), routes, pltpu.SemaphoreType.DMA((8,))]
    box_outs = [
        (VMEM, out(group, 4 + slots, SUB, LANES)),
        (HBM, out(*box_shape)),
        (VMEM, out(SUB, LANES)),
    ]
    norms = []
    table = None
    for cycle in range(CYCLES):
        first = cycle == 0
        body = fine_body((group, slots, nby, nbz, size_z), first)
        if first:
            ret, state, squares, table, kept, f_rate = call(
                body,
                [(VMEM, got)] + [(HBM, value) for value in (f_source, f_shift, f_start)],
                box_outs
                + [(HBM, out(group, COLS * slots, dtype=jnp.int32))]
                + [(HBM, out(*box_shape))] * 2,
                box_scratch
                + [
                    pltpu.SMEM((group, LANES), F32),
                    pltpu.SMEM((group + 1,), jnp.int32),
                    pltpu.SemaphoreType.DMA((group,)),
                ]
                + [flat] * 3,
            )
        else:
            ret, state, squares = call(
                body,
                [(HBM, table), (VMEM, got)]
                + [(HBM, value) for value in (state, kept, f_rate)],
                box_outs,
                box_scratch,
            )
        back = exchange(ret)
        units = (WIDE - 1) * (nt + 1) + 1
        added, side_a, side_b = call(
            place_body((ex, nt, group, slots, size_y, size_z, nby, nbz)),
            [(HBM, table), (VMEM, back)],
            [(VMEM, out(ex, 2, nt + 1, SUB, LANES))] + [(VMEM, out(units, SUB, LANES))] * 2,
            [routes, pltpu.SemaphoreType.DMA],
        )
        xa, xb = swap("gx", side_a, side_b)
        more = cycle < CYCLES - 1
        wide_shape = (span, 2, SUB * (nt + 1), LANES)
        result = call(
            coarse_body((ex, nt, group, slots, size_z), more),
            [(HBM, table)]
            + [(VMEM, v) for v in (wide, rate, source_wide, added, xa, xb, squares, *norms)],
            [
                (VMEM, out(ex, nt, SUB, LANES)),
                (VMEM, out(group, 4 if more else 5, SUB, LANES)),
                (VMEM, out(SUB, LANES)),
            ]
            + [(VMEM, out(1, WIDE, nt, SUB, LANES))] * (2 if more else 0),
            [pltpu.VMEM(wide_shape, F32)] * 3 + [routes, pltpu.SemaphoreType.DMA],
        )
        potential, send = result[:2]
        norms.append(result[2])
        got = exchange(send)
        if more:
            (wide,) = halos([potential], result[3], result[4], 1)
    (total,) = call(norm_body(group), [(VMEM, got)], [(VMEM, out(SUB, LANES))])
    (values,) = call(
        last_body((group, slots, size_z)),
        [(HBM, table), (VMEM, got), (HBM, state)],
        [(HBM, out(slots * fine // LANES, LANES))],
        [packs, ghost, whole, flat, routes, pltpu.SemaphoreType.DMA((3,))],
    )
    cells = float(ex * ey * ez * size_x * size_y * size_z)
    bit = 1
    while bit < size_x:
        pairs = [(i, i ^ bit) for i in range(size_x)]
        total = total + lax.ppermute(total, "gx", pairs)
        bit *= 2
    total = jnp.sum(total[:CYCLES], axis=1)
    values = values.reshape(fine // LANES, slots, LANES).transpose(1, 0, 2).reshape(slots, fine)
    return potential.reshape(ex, ey, ez), values, jnp.sqrt(total / cells)


def solution(mesh):
    in_specs = (
        P("gx", "gy", "gz"),
        P("gx", "gy", "gz"),
        P("gx", "gy", "gz"),
        P(("gx", "gy", "gz"), None),
        P(("gx", "gy", "gz"), None),
        P(("gx", "gy", "gz"), None),
        P(("gx", "gy", "gz"), None, None),
        P(("gx", "gy", "gz"), None),
    )
    out_specs = (P("gx", "gy", "gz"), P(("gx", "gy", "gz"), None), P())
    return jax.shard_map(work, mesh=mesh, in_specs=in_specs, out_specs=out_specs, check_vma=False)
```
